128 devices in a mesh: rows: 32 (over z, y, core), vecs: 4 (over x).
Axes of the slice: x: 4, y: 4, z: 4, core: 2. Of those that a mesh axis runs over, the one named last changes fastest.
Arguments:
- basis: bfloat16 [100, 2097152], P('vecs', 'rows'), may hold values from -6 to 6
- coefficients: bfloat16 [100, 40], replicated, may hold values from -0.625 to 0.625
- eigen_values: float32 [40], P('vecs'), may hold values from -3 to 1
- stiffness: float32 [2097152], P('rows'), may hold values from 6.5 to 10
- damping: float32 [2097152], P('rows'), may hold values from 0.2 to 2
- mass: float32 [2097152], P('rows'), may hold values from 0.5 to 2
- link_count: int32 [32], P('rows'), may hold values from 1024 to 4096, as said below
- lower_cells: int32 [32, 4096], P('rows'), may hold values from 0 to 4095
- upper_cells: int32 [32, 4096], P('rows'), may hold values from 0 to 4095
Outputs:
- eigvecs: bfloat16 [40, 2097152], P('vecs', 'rows')
- residuals: bfloat16 [40, 2097152], P('vecs', 'rows')
- relative_norms: float32 [40], P('vecs')
The draws below stay inside these ranges and needn't reach their ends.
Inputs may be any that keep to these rules, and one draw needn't show every extreme that they name: Interface s joins subdomain s to subdomain (s + 1) mod 32; only its first link_count[s] slots are used, the others are to be ignored. Some interface uses all 4096 slots in every draw. `lower_cells`: slots beyond link_count[s] hold values that are not used. `upper_cells`: slots beyond link_count[s] hold values that are not used.
All inputs are finite; a program needn't handle non-finite values.
Results may differ from the reference program's by a relative error of at most 0.0037.
The reference program's roundings to bfloat16 on the way count: a program that leaves them out, or rounds other values in their place, can miss the bound.
Values may be sent and summed in bfloat16 or wider, within the bound.
A program may use at most 320 MiB of HBM per device.

```python
import math
import jax
import jax.numpy as jnp
from jax import lax

RANK = 100
NV = 40
WID = 64
ZD = 16
HMAX = 4096
NSUB = 32
NROWS = 2097152
N_ROWS = 32


def draw_link_count(key, part):
    first_key, second_key = jax.random.split(jax.random.fold_in(key, 17))
    counts = jax.random.randint(first_key, (NSUB,), HMAX // 4, HMAX + 1)
    chosen = jax.random.randint(second_key, (), 0, NSUB)
    return jnp.where(jnp.arange(NSUB) == chosen, HMAX, counts).astype(jnp.int32)


def place_ends(array, key, least, largest):
    shape = array.shape
    place = [jax.random.randint(jax.random.fold_in(key, axis), (), 0, shape[axis]) for axis in range(len(shape))]
    array = array.at[tuple(place)].set(least)
    longest = shape.index(max(shape))
    place[longest] = (place[longest] + 1) % shape[longest]
    return array.at[tuple(place)].set(largest)


def block_levels(rng, dims, cuts, smallest, top_value):
    gain, own = 1.0, jax.random.fold_in(rng, 6)
    for dim, blocks in cuts:
        steps = jnp.exp(jax.random.uniform(jax.random.fold_in(own, dim), (blocks,), jnp.float32, smallest / len(cuts), top_value / len(cuts)))
        gain = gain * jnp.repeat(steps, dims[dim] // blocks).reshape([-1 if axis == dim else 1 for axis in range(len(dims))])
    return gain


def scatter_about(stream_key, dims, deviation, reach, cuts=(), held_as=jnp.bfloat16):
    result = deviation * jax.random.normal(stream_key, dims, jnp.float32)
    if cuts:
        result = result * block_levels(stream_key, dims, cuts, -0.22, 0.18)
    return jnp.clip(result, -reach, reach).astype(held_as)


def setup_inputs(seed: int = 0) -> dict:
    keys = jax.random.split(jax.random.key(seed), 10)
    basis = scatter_about(keys[0], (RANK, NROWS), 1.0, 6.0, ((0, 4), (1, 32)))
    coefficients = scatter_about(keys[1], (RANK, NV), RANK ** -0.5, 0.625)
    eigen_values = jnp.clip(-3.0 + 4.0 * jax.random.uniform(keys[2], (NV,), jnp.float32) ** block_levels(keys[2], (NV,), ((0, 4),), -0.2, 0.2), -3.0, 1.0)
    stiffness = jnp.clip(6.5 + 3.5 * jax.random.uniform(keys[3], (NROWS,), jnp.float32) ** block_levels(keys[3], (NROWS,), ((0, 32),), -0.2, 0.2), 6.5, 10.0)
    damping = jnp.clip(0.2 + 1.8 * jax.random.uniform(keys[4], (NROWS,), jnp.float32) ** block_levels(keys[4], (NROWS,), ((0, 32),), -0.2, 0.2), 0.2, 2.0)
    mass = jnp.clip(jnp.exp(math.log(2.0) - 1.3862944 * jax.random.uniform(keys[5], (NROWS,), jnp.float32) ** block_levels(keys[5], (NROWS,), ((0, 32),), -0.2, 0.2)), 0.5, 2.0)
    link_count = draw_link_count(jax.random.fold_in(keys[9], 71), 0)
    lower_cells = place_ends(jax.random.randint(keys[7], (NSUB, HMAX), 0, WID * WID), jax.random.fold_in(keys[7], 1), 0, (WID * WID) - 1).astype(jnp.int32)
    upper_cells = place_ends(jax.random.randint(keys[8], (NSUB, HMAX), 0, WID * WID), jax.random.fold_in(keys[8], 1), 0, (WID * WID) - 1).astype(jnp.int32)
    return {"basis": basis, "coefficients": coefficients, "eigen_values": eigen_values, "stiffness": stiffness, "damping": damping, "mass": mass, "link_count": link_count, "lower_cells": lower_cells, "upper_cells": upper_cells}


def neighbours(values, width_cells):
    depth_pad = jnp.pad(values, ((0, 0), (1, 1), (0, 0)))
    total = depth_pad[:, 2:] + depth_pad[:, :-2]
    across = jnp.pad(values, ((0, 0), (0, 0), (width_cells, width_cells)))
    total = total + across[:, :, 2 * width_cells:] + across[:, :, :-2 * width_cells]
    column = jnp.arange(values.shape[2]) % width_cells
    shifted = jnp.pad(values, ((0, 0), (0, 0), (1, 1)))
    total = total + jnp.where(column < width_cells - 1, shifted[:, :, 2:], 0.0)
    total = total + jnp.where(column > 0, shifted[:, :, :-2], 0.0)
    return total

def reference(basis, coefficients, eigen_values, stiffness, damping, mass, link_count, lower_cells, upper_cells):
    eigvecs = jnp.dot(coefficients.T, basis, preferred_element_type=jnp.float32).astype(jnp.bfloat16)
    vectors = eigvecs.astype(jnp.float32)
    plane_cells = WID * WID
    rows_local = ZD * plane_cells
    subdomains = N_ROWS
    neighbour_sum = neighbours(vectors.reshape(NV * subdomains, ZD, plane_cells), WID).reshape(NV, subdomains * rows_local)
    index_sub = jnp.arange(subdomains, dtype=jnp.int32)[:, None]
    lower_rows = (index_sub * rows_local + (ZD - 1) * plane_cells + lower_cells).reshape(-1).astype(jnp.int32)
    upper_rows = ((index_sub + 1) % subdomains * rows_local + upper_cells).reshape(-1).astype(jnp.int32)
    slot_used = (jnp.arange(HMAX, dtype=jnp.int32)[None, :] < link_count[:, None]).astype(jnp.float32).reshape(-1)
    link_sum = jnp.zeros_like(vectors)
    link_sum = link_sum.at[:, lower_rows].add(vectors[:, upper_rows] * slot_used)
    link_sum = link_sum.at[:, upper_rows].add(vectors[:, lower_rows] * slot_used)
    eigen_col = eigen_values[:, None]
    diagonal = eigen_col * eigen_col * mass[None, :] + eigen_col * damping[None, :] + stiffness[None, :]
    coupling = eigen_col * eigen_col * 0.1 + eigen_col * 0.3 + 1.0
    residual_full = diagonal * vectors - coupling * (neighbour_sum + link_sum)
    vector_sq = lax.optimization_barrier(jnp.sum(vectors * vectors, axis=1))
    residual_sq = lax.optimization_barrier(jnp.sum(residual_full * residual_full, axis=1))
    relative_norms = jnp.sqrt(residual_sq) / jnp.sqrt(vector_sq + 1.0)
    return (eigvecs, residual_full.astype(jnp.bfloat16), relative_norms)
```

```python
import functools

import jax
import jax.numpy as jnp
from jax import lax
from jax.experimental import pallas as pl
from jax.experimental.pallas import tpu as pltpu
from jax.sharding import PartitionSpec as P

WID = 64
LANES = 128
CHUNKS = 8
DEPTH = 32
PAD = 16
BLOCK = 512
LEAD = 6
LAG = 2
LINKS_AT = 7


def remote(src, dst, send_sem, recv_sem, where):
    return pltpu.make_async_remote_copy(
        src_ref=src,
        dst_ref=dst,
        send_sem=send_sem,
        recv_sem=recv_sem,
        device_id=where,
        device_id_type=pl.DeviceIdType.MESH,
    )


def iota(shape, axis):
    return lax.broadcasted_iota(jnp.int32, shape, axis)


def ones_where(condition):
    return jnp.where(condition, 1.0, 0.0).astype(jnp.bfloat16)


def kernel(
    count,
    planes,
    cells,
    vector_part,
    rank_part,
    basis,
    coefficients_in,
    eigen_in,
    stiffness_in,
    damping_in,
    mass_in,
    used_in,
    lower_in,
    upper_in,
    eig_out,
    res_out,
    norm_out,
    own_basis,
    first_out,
    first_in,
    along_out,
    along_in,
    back_out,
    back_in,
    middle,
    values,
    packed,
    res_packed,
    face_in,
    links_in,
    links,
    link_sums,
    stat_out,
    stat_in,
    stat_line,
    factors,
    spread_rows,
    chunk_ones,
    lam_of,
    stiffness,
    damping,
    mass,
    coefficients,
    eigen,
    used,
    lower,
    upper,
    input_sem,
    local_sem,
    first_send,
    first_recv,
    along_send,
    along_recv,
    back_send,
    back_recv,
    face_send,
    face_recv,
    stat_send,
    stat_recv,
):
    row = lax.axis_index("rows")
    vec = lax.axis_index("vecs")
    vecs = 4
    above = {"rows": (row + 1) % count}
    below = {"rows": (row + count - 1) % count}
    slots = links.shape[1] // 2
    width = cells // CHUNKS
    parts = width // LANES
    held = vector_part * CHUNKS
    plane_rows = cells // LANES

    def plane_at(step):
        return (step + planes - 1) % planes

    def toward(step):
        return {"vecs": (vec + 1 + 2 * (step % 2)) % vecs}

    def away(step):
        return {"vecs": (vec + 3 - 2 * (step % 2)) % vecs}

    def local_copy(step):
        start = pl.multiple_of(plane_at(step) * cells, cells)
        return pltpu.make_async_copy(
            basis.at[:, pl.ds(start, cells)],
            own_basis.at[step],
            local_sem.at[step],
        )

    def first_copy(step):
        return remote(
            first_out.at[step],
            first_in.at[step],
            first_send.at[step],
            first_recv.at[step],
            toward(step),
        )

    def along_copy(step):
        return remote(
            along_out.at[step],
            along_in.at[step],
            along_send.at[step],
            along_recv.at[step],
            toward(step),
        )

    def back_copy(step):
        return remote(
            back_out.at[step],
            back_in.at[step],
            back_send.at[step],
            back_recv.at[step],
            away(step),
        )

    def face_copy(which):
        return remote(
            packed.at[which],
            face_in.at[which],
            face_send.at[which],
            face_recv.at[which],
            above if which == 0 else below,
        )

    def links_copy():
        return remote(links, links_in, face_send.at[2], face_recv.at[2], above)

    def stat_copy(step):
        return remote(
            stat_line,
            stat_in.at[step],
            stat_send.at[step],
            stat_recv.at[step],
            {"rows": (row + step) % count},
        )

    def each(first, last, body):
        def run(step, carry):
            body(step)
            return carry

        lax.fori_loop(first, last, run, 0)

    barrier = pltpu.get_barrier_semaphore()

    def greet(where):
        pl.semaphore_signal(barrier, inc=1, device_id=where, device_id_type=pl.DeviceIdType.MESH)

    coefficients_copy = pltpu.make_async_copy(coefficients_in, coefficients, input_sem.at[0])
    coefficients_copy.start()
    each(0, planes, lambda step: local_copy(step).start())
    inputs = [
        pltpu.make_async_copy(source, target, input_sem.at[place + 1])
        for place, (source, target) in enumerate(
            (
                (eigen_in, eigen),
                (used_in, used),
                (lower_in, lower),
                (upper_in, upper),
                (stiffness_in, stiffness),
                (damping_in, damping),
                (mass_in, mass),
            )
        )
    ]
    for copy in inputs:
        copy.start()
    greet({"vecs": (vec + 1) % vecs})
    greet({"vecs": (vec + 3) % vecs})
    each(1, count, lambda step: greet({"rows": (row + step) % count}))

    coefficients_copy.wait()
    total_rank, total_vectors = coefficients.shape[1], coefficients.shape[0]
    rank = iota((total_rank, CHUNKS * DEPTH), 0)
    deep = iota((total_rank, CHUNKS * DEPTH), 1) & (DEPTH - 1)
    pick = ones_where((rank == vec * rank_part + deep) & (deep < rank_part))
    own_rank = jnp.dot(coefficients[...], pick, preferred_element_type=jnp.float32)
    own_rank = own_rank.astype(jnp.bfloat16)
    same_chunk = (iota((held, CHUNKS * DEPTH), 0) & (CHUNKS - 1)) == (
        iota((held, CHUNKS * DEPTH), 1) // DEPTH
    )
    vector = iota((held, total_vectors), 1)
    vector_of = iota((held, total_vectors), 0) // CHUNKS
    for place, ahead in enumerate((2, 1, 0, 3)):
        owner = (vec + ahead) % vecs
        choose = ones_where(vector == owner * vector_part + vector_of)
        part = jnp.dot(choose, own_rank, preferred_element_type=jnp.float32)
        part = jnp.where(same_chunk, part, 0.0).astype(jnp.bfloat16)
        factors[0, place * held : (place + 1) * held] = part
        place = place if place % 2 == 0 else 4 - place
        factors[1, place * held : (place + 1) * held] = part

    unused = jnp.zeros((DEPTH - rank_part, width), jnp.bfloat16)

    def produce(step):
        local_copy(step).wait()
        pieces = []
        for chunk in range(CHUNKS):
            piece = own_basis[step, :, chunk * width : (chunk + 1) * width]
            pieces += [piece, unused]
        stacked = jnp.concatenate(pieces, axis=0)
        role = step % 2

        def part(place):
            return jnp.dot(
                factors[role, place * held : (place + 1) * held],
                stacked,
                preferred_element_type=jnp.float32,
            )

        first_out[step] = part(0).astype(jnp.bfloat16)
        first_copy(step).start()
        middle[step] = part(1)
        values[plane_at(step) + 1] = part(2)
        back_out[step] = part(3).astype(jnp.bfloat16)

    def relay(step):
        first_copy(step).wait_recv()
        for start in range(0, held, PAD):
            rows = slice(start, start + PAD)
            total = middle[step, rows] + first_in[step, rows].astype(jnp.float32)
            along_out[step, rows] = total.astype(jnp.bfloat16)
        along_copy(step).start()
        back_copy(step).start()

    pl.semaphore_wait(barrier, count + 1)
    each(0, LEAD, produce)

    for copy in inputs:
        copy.wait()
    values[0] = jnp.zeros((held, width), jnp.float32)
    values[planes + 1] = jnp.zeros((held, width), jnp.float32)
    stat_out[...] = jnp.zeros_like(stat_out)
    link_sums[...] = jnp.zeros_like(link_sums)

    is_used = iota((1, slots), 1) < used[0]
    links[:, :slots] = jnp.where(is_used, lower[...], -1)
    links[:, slots:] = jnp.where(is_used, upper[...], -1)
    links_copy().start()

    place = iota((CHUNKS * PAD, held), 0)
    source = iota((CHUNKS * PAD, held), 1)
    spread_rows[...] = ones_where(
        ((place // PAD) == (source & (CHUNKS - 1))) & ((place & (PAD - 1)) == (source // CHUNKS))
    )
    chunk_ones[...] = ones_where(
        (iota((held, held), 0) // CHUNKS) == (iota((held, held), 1) // CHUNKS)
    )
    diag = (iota((held, vector_part), 0) // CHUNKS) == iota((held, vector_part), 1)
    lam = jnp.where(diag, jnp.broadcast_to(eigen[...], (held, vector_part)), 0.0)
    lam = jnp.broadcast_to(jnp.sum(lam, axis=1, keepdims=True), (held, LANES))
    lam_of[0] = lam
    lam_of[1] = lam * lam
    lam_of[2] = lam * lam * 0.1 + lam * 0.3 + 1.0

    def fold(block):
        total = block[:, :LANES]
        for start in range(LANES, block.shape[1], LANES):
            total = total + block[:, start : start + LANES]
        return total

    def write(out, plane, block):
        moved = jnp.dot(spread_rows[...], block, preferred_element_type=jnp.float32)
        for chunk in range(CHUNKS):
            start = pl.multiple_of(plane * cells + chunk * width, width)
            piece = moved[chunk * PAD : (chunk + 1) * PAD].astype(jnp.bfloat16)
            out[:, pl.ds(start, width)] = piece[:vector_part]

    def finish(step):
        plane = plane_at(step)
        along_copy(step).wait_recv()
        back_copy(step).wait_recv()
        for start in range(0, held, PAD):
            rows = slice(start, start + PAD)
            total = values[plane + 1, rows] + along_in[step, rows].astype(jnp.float32)
            total = total + back_in[step, rows].astype(jnp.float32)
            rounded = total.astype(jnp.bfloat16)
            exact = rounded.astype(jnp.float32)
            values[plane + 1, rows] = exact
            packed[step, rows] = rounded
            stat_out[rows] += fold(exact * exact)
        write(eig_out, plane, packed[step])

    column = iota((PAD, LANES), 1)
    not_left = (column & (WID - 1)) != 0
    not_right = (column & (WID - 1)) != WID - 1
    low_half = column < WID
    chunk_of = iota((PAD, LANES), 0) & (CHUNKS - 1)
    not_first = chunk_of != 0
    not_last = chunk_of != CHUNKS - 1

    def stencil(plane, link):
        diagonals = []
        for part in range(parts):
            at = pl.ds(plane * plane_rows + part, CHUNKS, stride=parts)
            diagonals.append(
                [jnp.concatenate([array[at]] * 2, axis=0) for array in (mass, damping, stiffness)]
            )
        for start in range(0, held, PAD):
            rows = slice(start, start + PAD)
            lam = lam_of[0, rows]
            lam_sq = lam_of[1, rows]
            coupling = lam_of[2, rows]
            mids = [
                values[plane + 1, rows, part * LANES : (part + 1) * LANES] for part in range(parts)
            ]
            swapped = [pltpu.roll(mid, WID, 1) for mid in mids]
            before = jnp.where(not_first, pltpu.roll(swapped[-1], 1, 0), 0.0)
            after = jnp.where(not_last, pltpu.roll(swapped[0], PAD - 1, 0), 0.0)
            swapped = [before, *swapped, after]
            squares = jnp.zeros((PAD, LANES), jnp.float32)
            for part in range(parts):
                lanes = slice(part * LANES, (part + 1) * LANES)
                mid = mids[part]
                total = values[plane, rows, lanes] + values[plane + 2, rows, lanes]
                total = total + (
                    swapped[part + 1] + jnp.where(low_half, swapped[part], swapped[part + 2])
                )
                total = total + jnp.where(not_right, pltpu.roll(mid, LANES - 1, 1), 0.0)
                total = total + jnp.where(not_left, pltpu.roll(mid, 1, 1), 0.0)
                if link is not None:
                    at = part * held + start
                    total = total + link_sums[link, at : at + PAD]
                mass_b, damping_b, stiffness_b = diagonals[part]
                diagonal = lam_sq * mass_b + lam * damping_b + stiffness_b
                full = diagonal * mid - coupling * total
                res_packed[rows, lanes] = full.astype(jnp.bfloat16)
                squares = squares + full * full
            at = slice(held + start, held + start + PAD)
            stat_out[at] += squares
        write(res_out, plane, res_packed[...])

    low_iota = iota((LANES, BLOCK), 0)
    row_chunk = iota((held, BLOCK), 0) & (CHUNKS - 1)

    def link_side(which, lists, source_row, target_row, step):
        stacked = jnp.concatenate(
            [face_in[which, :, part * LANES : (part + 1) * LANES] for part in range(parts)], axis=0
        )
        source = lists[:, pl.ds(pl.multiple_of(source_row * slots + step * BLOCK, BLOCK), BLOCK)]
        target = lists[:, pl.ds(pl.multiple_of(target_row * slots + step * BLOCK, BLOCK), BLOCK)]
        low = ones_where(low_iota == (source & (LANES - 1)))
        picked = jnp.dot(stacked, low, preferred_element_type=jnp.float32)
        high = jnp.broadcast_to(source >> 7, (held, BLOCK))
        got = jnp.zeros((held, BLOCK), jnp.float32)
        for part in range(parts):
            mine = high == row_chunk * parts + part
            got = got + jnp.where(mine, picked[part * held : (part + 1) * held], 0.0)
        got = jnp.dot(
            chunk_ones[...], got.astype(jnp.bfloat16), preferred_element_type=jnp.float32
        )
        high = jnp.broadcast_to(target >> 7, (held, BLOCK))
        placed = jnp.concatenate(
            [
                jnp.where(high == row_chunk * parts + part, got, 0.0).astype(jnp.bfloat16)
                for part in range(parts)
            ],
            axis=0,
        )
        low = ones_where(low_iota == (target & (LANES - 1)))
        link_sums[which] += lax.dot_general(
            placed, low, (((1,), (1,)), ((), ())), preferred_element_type=jnp.float32
        )

    def advance(step):
        @pl.when(step + LEAD < planes)
        def _():
            produce(step + LEAD)

        @pl.when(step < planes)
        def _():
            relay(step)

        @pl.when(step >= LAG)
        def _():
            finish(step - LAG)

            @pl.when(step == LAG)
            def _():
                face_copy(0).start()

            @pl.when(step == LAG + 1)
            def _():
                face_copy(1).start()

        @pl.when(step >= LAG + 3)
        def _():
            stencil(step - LAG - 2, None)

        @pl.when(step == LINKS_AT)
        def _():
            face_copy(0).wait_recv()
            face_copy(1).wait_recv()
            links_copy().wait_recv()

        @pl.when((step >= LINKS_AT) & (step < LINKS_AT + slots // BLOCK))
        def _():
            link_side(0, links_in, 0, 1, step - LINKS_AT)
            link_side(1, links, 1, 0, step - LINKS_AT)

        @pl.when(step == LINKS_AT + slots // BLOCK)
        def _():
            stencil(0, 0)

    each(0, planes + LAG, advance)
    stencil(planes - 2, None)
    stencil(planes - 1, 1)

    sums = jnp.sum(stat_out[...].reshape(2 * vector_part, CHUNKS, LANES), axis=1)
    sums = jnp.sum(sums, axis=1, keepdims=True)
    spot = iota((2 * vector_part, LANES), 0) == iota((2 * vector_part, LANES), 1)
    line = jnp.sum(jnp.where(spot, sums, 0.0), axis=0, keepdims=True)
    stat_line[...] = line
    each(1, count, lambda step: stat_copy(step).start())

    def sent(step):
        first_copy(step).wait_send()
        along_copy(step).wait_send()
        back_copy(step).wait_send()

    each(0, planes, sent)
    links_copy().wait_send()
    face_copy(0).wait_send()
    face_copy(1).wait_send()
    each(1, count, lambda step: stat_copy(step).wait_recv())
    for step in range(1, count):
        line = line + stat_in[step]
    norms = jnp.sqrt(line[:, vector_part : 2 * vector_part]) / jnp.sqrt(line[:, :vector_part] + 1.0)
    norm_out[...] = norms
    each(1, count, lambda step: stat_copy(step).wait_send())


def write_back(eig_held, res_held, norm_held, eig_out, res_out, norm_out, sem):
    copies = [
        pltpu.make_async_copy(source, target, sem.at[place])
        for place, (source, target) in enumerate(
            ((eig_held, eig_out), (res_held, res_out), (norm_held, norm_out))
        )
    ]
    for copy in copies:
        copy.start()
    for copy in copies:
        copy.wait()


def on_device(
    basis,
    coefficients,
    eigen_values,
    stiffness,
    damping,
    mass,
    link_count,
    lower_cells,
    upper_cells,
):
    count = lax.axis_size("rows")
    vector_part = eigen_values.shape[0]
    rank_part, rows_local = basis.shape
    cells = WID * WID
    planes = rows_local // cells
    slots = lower_cells.shape[1]
    held = vector_part * CHUNKS
    width = cells // CHUNKS
    vmem = pl.BlockSpec(memory_space=pltpu.VMEM)
    anywhere = pl.BlockSpec(memory_space=pltpu.HBM)
    dma = pltpu.SemaphoreType.DMA
    wire = pltpu.VMEM((planes, held, width), jnp.bfloat16)
    eigvecs, residuals, norms = pl.pallas_call(
        functools.partial(kernel, count, planes, cells, vector_part, rank_part),
        out_shape=(
            pltpu.VMEM((vector_part, rows_local), jnp.bfloat16),
            pltpu.VMEM((vector_part, rows_local), jnp.bfloat16),
            pltpu.VMEM((1, vector_part), jnp.float32),
        ),
        in_specs=[anywhere] * 9,
        out_specs=(vmem, vmem, vmem),
        scratch_shapes=[
            pltpu.VMEM((planes, rank_part, cells), jnp.bfloat16),
            wire,
            wire,
            wire,
            wire,
            wire,
            wire,
            pltpu.VMEM((planes, held, width), jnp.float32),
            pltpu.VMEM((planes + 2, held, width), jnp.float32),
            wire,
            pltpu.VMEM((held, width), jnp.bfloat16),
            pltpu.VMEM((2, held, width), jnp.bfloat16),
            pltpu.VMEM((1, 2 * slots), jnp.int32),
            pltpu.VMEM((1, 2 * slots), jnp.int32),
            pltpu.VMEM((2, width // LANES * held, LANES), jnp.float32),
            pltpu.VMEM((2 * held, LANES), jnp.float32),
            pltpu.VMEM((count, 1, LANES), jnp.float32),
            pltpu.VMEM((1, LANES), jnp.float32),
            pltpu.VMEM((2, 4 * held, CHUNKS * DEPTH), jnp.bfloat16),
            pltpu.VMEM((CHUNKS * PAD, held), jnp.bfloat16),
            pltpu.VMEM((held, held), jnp.bfloat16),
            pltpu.VMEM((3, held, LANES), jnp.float32),
            pltpu.VMEM((rows_local // LANES, LANES), jnp.float32),
            pltpu.VMEM((rows_local // LANES, LANES), jnp.float32),
            pltpu.VMEM((rows_local // LANES, LANES), jnp.float32),
            pltpu.VMEM(coefficients.shape[::-1], jnp.bfloat16),
            pltpu.VMEM((1, vector_part), jnp.float32),
            pltpu.SMEM((1,), jnp.int32),
            pltpu.VMEM((1, slots), jnp.int32),
            pltpu.VMEM((1, slots), jnp.int32),
            dma((8,)),
            dma((planes,)),
            dma((planes,)),
            dma((planes,)),
            dma((planes,)),
            dma((planes,)),
            dma((planes,)),
            dma((planes,)),
            dma((3,)),
            dma((3,)),
            dma((count,)),
            dma((count,)),
        ],
        compiler_params=pltpu.CompilerParams(
            collective_id=0, has_side_effects=True, vmem_limit_bytes=56 * 1024 * 1024
        ),
    )(
        basis,
        coefficients.T,
        eigen_values[None, :],
        stiffness.reshape(-1, LANES),
        damping.reshape(-1, LANES),
        mass.reshape(-1, LANES),
        link_count,
        lower_cells,
        upper_cells,
    )
    eigvecs, residuals, norms = pl.pallas_call(
        write_back,
        out_shape=tuple(
            jax.ShapeDtypeStruct(held.shape, held.dtype) for held in (eigvecs, residuals, norms)
        ),
        in_specs=[vmem] * 3,
        out_specs=[pl.BlockSpec(memory_space=pl.ANY)] * 3,
        scratch_shapes=[dma((3,))],
        compiler_params=pltpu.CompilerParams(vmem_limit_bytes=1 << 20),
    )(eigvecs, residuals, norms)
    return eigvecs, residuals, norms[0]


def solution(mesh):
    placed = (
        P("vecs", "rows"),
        P(),
        P("vecs"),
        P("rows"),
        P("rows"),
        P("rows"),
        P("rows"),
        P("rows", None),
        P("rows", None),
    )
    return jax.shard_map(
        on_device,
        mesh=mesh,
        in_specs=placed,
        out_specs=(P("vecs", "rows"), P("vecs", "rows"), P("vecs")),
        check_vma=False,
    )
```

```python
import functools

import jax
import jax.numpy as jnp
from jax import lax
from jax.experimental import pallas as pl
from jax.experimental.pallas import tpu as pltpu
from jax.sharding import PartitionSpec as P

WID = 64
LANES = 128
CHUNKS = 8
DEPTH = 32
PAD = 16
BLOCK = 512
LEAD = 6
LAG = 2
LINKS_AT = 6


def remote(src, dst, send_sem, recv_sem, where):
    return pltpu.make_async_remote_copy(
        src_ref=src,
        dst_ref=dst,
        send_sem=send_sem,
        recv_sem=recv_sem,
        device_id=where,
        device_id_type=pl.DeviceIdType.MESH,
    )


def iota(shape, axis):
    return lax.broadcasted_iota(jnp.int32, shape, axis)


def ones_where(condition):
    return jnp.where(condition, 1.0, 0.0).astype(jnp.bfloat16)


def kernel(
    count,
    planes,
    cells,
    vector_part,
    rank_part,
    basis,
    coefficients_in,
    eigen_in,
    stiffness_in,
    damping_in,
    mass_in,
    used_in,
    lower_in,
    upper_in,
    eig_out,
    res_out,
    norm_out,
    own_basis,
    first_out,
    first_in,
    along_out,
    along_in,
    back_out,
    back_in,
    middle,
    values,
    packed,
    res_packed,
    face_in,
    links_in,
    links,
    link_sums,
    stat_out,
    stat_in,
    stat_line,
    factors,
    spread_rows,
    chunk_ones,
    lam_of,
    stiffness,
    damping,
    mass,
    coefficients,
    eigen,
    used,
    lower,
    upper,
    input_sem,
    local_sem,
    first_send,
    first_recv,
    along_send,
    along_recv,
    back_send,
    back_recv,
    face_send,
    face_recv,
    stat_send,
    stat_recv,
    meet_sem,
):
    row = lax.axis_index("rows")
    vec = lax.axis_index("vecs")
    vecs = 4
    above = {"rows": (row + 1) % count}
    below = {"rows": (row + count - 1) % count}
    slots = links.shape[1] // 2
    width = cells // CHUNKS
    parts = width // LANES
    held = vector_part * CHUNKS
    plane_rows = cells // LANES

    def plane_at(step):
        return (step + planes - 1) % planes

    def toward(step):
        return {"vecs": (vec + 1 + 2 * (step % 2)) % vecs}

    def away(step):
        return {"vecs": (vec + 3 - 2 * (step % 2)) % vecs}

    def local_copy(step):
        start = pl.multiple_of(plane_at(step) * cells, cells)
        return pltpu.make_async_copy(
            basis.at[:, pl.ds(start, cells)],
            own_basis.at[step],
            local_sem.at[step],
        )

    def first_copy(step):
        return remote(
            first_out.at[step],
            first_in.at[step],
            first_send.at[step],
            first_recv.at[step],
            toward(step),
        )

    def along_copy(step):
        return remote(
            along_out.at[step],
            along_in.at[step],
            along_send.at[step],
            along_recv.at[step],
            toward(step),
        )

    def back_copy(step):
        return remote(
            back_out.at[step],
            back_in.at[step],
            back_send.at[step],
            back_recv.at[step],
            away(step),
        )

    def face_copy(which):
        return remote(
            packed.at[which],
            face_in.at[which],
            face_send.at[which],
            face_recv.at[which],
            above if which == 0 else below,
        )

    def links_copy():
        return remote(links, links_in, face_send.at[2], face_recv.at[2], above)

    def stat_copy(step):
        return remote(
            stat_line,
            stat_in.at[step],
            stat_send.at[step],
            stat_recv.at[step],
            {"rows": (row + step) % count},
        )

    def each(first, last, body):
        def run(step, carry):
            body(step)
            return carry

        lax.fori_loop(first, last, run, 0)

    barrier = pltpu.get_barrier_semaphore()

    def greet(where):
        pl.semaphore_signal(barrier, inc=1, device_id=where, device_id_type=pl.DeviceIdType.MESH)

    coefficients_copy = pltpu.make_async_copy(coefficients_in, coefficients, input_sem.at[0])
    coefficients_copy.start()
    each(0, planes, lambda step: local_copy(step).start())
    inputs = [
        pltpu.make_async_copy(source, target, input_sem.at[place + 1])
        for place, (source, target) in enumerate(
            (
                (eigen_in, eigen),
                (used_in, used),
                (lower_in, lower),
                (upper_in, upper),
                (stiffness_in, stiffness),
                (damping_in, damping),
                (mass_in, mass),
            )
        )
    ]
    for copy in inputs:
        copy.start()
    greet({"vecs": (vec + 1) % vecs})
    greet({"vecs": (vec + 3) % vecs})
    greet(above)
    greet(below)

    def meet(round_):
        for where in (row + 2**round_, row + count - 2**round_):
            pl.semaphore_signal(
                meet_sem.at[round_],
                inc=1,
                device_id={"rows": where % count},
                device_id_type=pl.DeviceIdType.MESH,
            )

    coefficients_copy.wait()
    total_rank, total_vectors = coefficients.shape[1], coefficients.shape[0]
    rank = iota((total_rank, CHUNKS * DEPTH), 0)
    deep = iota((total_rank, CHUNKS * DEPTH), 1) & (DEPTH - 1)
    pick = ones_where((rank == vec * rank_part + deep) & (deep < rank_part))
    own_rank = jnp.dot(coefficients[...], pick, preferred_element_type=jnp.float32)
    own_rank = own_rank.astype(jnp.bfloat16)
    same_chunk = (iota((held, CHUNKS * DEPTH), 0) & (CHUNKS - 1)) == (
        iota((held, CHUNKS * DEPTH), 1) // DEPTH
    )
    vector = iota((held, total_vectors), 1)
    vector_of = iota((held, total_vectors), 0) // CHUNKS
    for place, ahead in enumerate((2, 1, 0, 3)):
        owner = (vec + ahead) % vecs
        choose = ones_where(vector == owner * vector_part + vector_of)
        part = jnp.dot(choose, own_rank, preferred_element_type=jnp.float32)
        part = jnp.where(same_chunk, part, 0.0).astype(jnp.bfloat16)
        factors[0, place * held : (place + 1) * held] = part
        place = place if place % 2 == 0 else 4 - place
        factors[1, place * held : (place + 1) * held] = part

    unused = jnp.zeros((DEPTH - rank_part, width), jnp.bfloat16)

    def produce(step):
        local_copy(step).wait()
        pieces = []
        for chunk in range(CHUNKS):
            piece = own_basis[step, :, chunk * width : (chunk + 1) * width]
            pieces += [piece, unused]
        stacked = jnp.concatenate(pieces, axis=0)
        role = step % 2

        def part(place):
            return jnp.dot(
                factors[role, place * held : (place + 1) * held],
                stacked,
                preferred_element_type=jnp.float32,
            )

        first_out[step] = part(0).astype(jnp.bfloat16)
        first_copy(step).start()
        middle[step] = part(1)
        values[plane_at(step) + 1] = part(2)
        back_out[step] = part(3).astype(jnp.bfloat16)

    def relay(step):
        first_copy(step).wait_recv()
        for start in range(0, held, PAD):
            rows = slice(start, start + PAD)
            total = middle[step, rows] + first_in[step, rows].astype(jnp.float32)
            along_out[step, rows] = total.astype(jnp.bfloat16)
        along_copy(step).start()
        back_copy(step).start()

    pl.semaphore_wait(barrier, 4)
    meet(0)
    each(0, LEAD, produce)

    for copy in inputs:
        copy.wait()
    values[0] = jnp.zeros((held, width), jnp.float32)
    values[planes + 1] = jnp.zeros((held, width), jnp.float32)
    stat_out[...] = jnp.zeros_like(stat_out)
    link_sums[...] = jnp.zeros_like(link_sums)

    is_used = iota((1, slots), 1) < used[...]
    links[:, :slots] = jnp.where(is_used, lower[...], -1)
    links[:, slots:] = jnp.where(is_used, upper[...], -1)
    links_copy().start()

    place = iota((CHUNKS * PAD, held), 0)
    source = iota((CHUNKS * PAD, held), 1)
    spread_rows[...] = ones_where(
        ((place // PAD) == (source & (CHUNKS - 1))) & ((place & (PAD - 1)) == (source // CHUNKS))
    )
    chunk_ones[...] = ones_where(
        (iota((held, held), 0) // CHUNKS) == (iota((held, held), 1) // CHUNKS)
    )
    diag = (iota((held, vector_part), 0) // CHUNKS) == iota((held, vector_part), 1)
    lam = jnp.where(diag, jnp.broadcast_to(eigen[...], (held, vector_part)), 0.0)
    lam = jnp.broadcast_to(jnp.sum(lam, axis=1, keepdims=True), (held, LANES))
    lam_of[0] = lam
    lam_of[1] = lam * lam
    lam_of[2] = lam * lam * 0.1 + lam * 0.3 + 1.0

    def fold(block):
        total = block[:, :LANES]
        for start in range(LANES, block.shape[1], LANES):
            total = total + block[:, start : start + LANES]
        return total

    def write(out, plane, block):
        moved = jnp.dot(spread_rows[...], block, preferred_element_type=jnp.float32)
        for chunk in range(CHUNKS):
            start = pl.multiple_of(plane * cells + chunk * width, width)
            piece = moved[chunk * PAD : (chunk + 1) * PAD].astype(jnp.bfloat16)
            out[:, pl.ds(start, width)] = piece[:vector_part]

    def finish(step):
        plane = plane_at(step)
        along_copy(step).wait_recv()
        back_copy(step).wait_recv()
        for start in range(0, held, PAD):
            rows = slice(start, start + PAD)
            total = values[plane + 1, rows] + along_in[step, rows].astype(jnp.float32)
            total = total + back_in[step, rows].astype(jnp.float32)
            rounded = total.astype(jnp.bfloat16)
            exact = rounded.astype(jnp.float32)
            values[plane + 1, rows] = exact
            packed[step, rows] = rounded
            stat_out[rows] += fold(exact * exact)

    def write_eig(step):
        write(eig_out, plane_at(step), packed[step])

    def write_res(plane, slot):
        write(res_out, plane, res_packed[slot])

    column = iota((PAD, LANES), 1)
    not_left = (column & (WID - 1)) != 0
    not_right = (column & (WID - 1)) != WID - 1
    low_half = column < WID
    chunk_of = iota((PAD, LANES), 0) & (CHUNKS - 1)
    not_first = chunk_of != 0
    not_last = chunk_of != CHUNKS - 1

    def stencil(plane, link, slot=0):
        diagonals = []
        for part in range(parts):
            at = pl.ds(plane * plane_rows + part, CHUNKS, stride=parts)
            diagonals.append(
                [jnp.concatenate([array[at]] * 2, axis=0) for array in (mass, damping, stiffness)]
            )
        for start in range(0, held, PAD):
            rows = slice(start, start + PAD)
            lam = lam_of[0, rows]
            lam_sq = lam_of[1, rows]
            coupling = lam_of[2, rows]
            mids = [
                values[plane + 1, rows, part * LANES : (part + 1) * LANES] for part in range(parts)
            ]
            swapped = [pltpu.roll(mid, WID, 1) for mid in mids]
            before = jnp.where(not_first, pltpu.roll(swapped[-1], 1, 0), 0.0)
            after = jnp.where(not_last, pltpu.roll(swapped[0], PAD - 1, 0), 0.0)
            swapped = [before, *swapped, after]
            squares = jnp.zeros((PAD, LANES), jnp.float32)
            for part in range(parts):
                lanes = slice(part * LANES, (part + 1) * LANES)
                mid = mids[part]
                total = values[plane, rows, lanes] + values[plane + 2, rows, lanes]
                total = total + (
                    swapped[part + 1] + jnp.where(low_half, swapped[part], swapped[part + 2])
                )
                total = total + jnp.where(not_right, pltpu.roll(mid, LANES - 1, 1), 0.0)
                total = total + jnp.where(not_left, pltpu.roll(mid, 1, 1), 0.0)
                if link is not None:
                    at = part * held + start
                    total = total + link_sums[link, at : at + PAD]
                mass_b, damping_b, stiffness_b = diagonals[part]
                diagonal = lam_sq * mass_b + lam * damping_b + stiffness_b
                full = diagonal * mid - coupling * total
                res_packed[slot, rows, lanes] = full.astype(jnp.bfloat16)
                squares = squares + full * full
            at = slice(held + start, held + start + PAD)
            stat_out[at] += squares

    low_iota = iota((LANES, BLOCK), 0)
    row_chunk = iota((held, BLOCK), 0) & (CHUNKS - 1)

    sides = ((0, links_in, 0, 1), (1, links, 1, 0))

    def link_block(step):
        start = pl.multiple_of(step * BLOCK, BLOCK)
        targets, picked, got = [], [], []
        for which, lists, source_row, target_row in sides:
            stacked = jnp.concatenate(
                [face_in[which, :, part * LANES : (part + 1) * LANES] for part in range(parts)],
                axis=0,
            )
            source = lists[:, pl.ds(source_row * slots + start, BLOCK)]
            targets.append(lists[:, pl.ds(target_row * slots + start, BLOCK)])
            low = ones_where(low_iota == (source & (LANES - 1)))
            rows = jnp.dot(stacked, low, preferred_element_type=jnp.float32)
            picked.append((source, rows))
        for source, rows in picked:
            high = jnp.broadcast_to(source >> 7, (held, BLOCK))
            total = jnp.zeros((held, BLOCK), jnp.float32)
            for part in range(parts):
                mine = high == row_chunk * parts + part
                total = total + jnp.where(mine, rows[part * held : (part + 1) * held], 0.0)
            got.append(
                jnp.dot(
                    chunk_ones[...], total.astype(jnp.bfloat16), preferred_element_type=jnp.float32
                )
            )
        for (which, *_), target, value in zip(sides, targets, got):
            high = jnp.broadcast_to(target >> 7, (held, BLOCK))
            placed = jnp.concatenate(
                [
                    jnp.where(high == row_chunk * parts + part, value, 0.0).astype(jnp.bfloat16)
                    for part in range(parts)
                ],
                axis=0,
            )
            low = ones_where(low_iota == (target & (LANES - 1)))
            link_sums[which] += lax.dot_general(
                placed, low, (((1,), (1,)), ((), ())), preferred_element_type=jnp.float32
            )

    rounds = meet_sem.shape[0]

    def advance(step):
        for round_ in range(rounds):

            @pl.when(step == 2 * round_ + 1)
            def _():
                pl.semaphore_wait(meet_sem.at[round_], 2)
                if round_ + 1 < rounds:
                    meet(round_ + 1)

        @pl.when(step + LEAD < planes)
        def _():
            produce(step + LEAD)

        @pl.when(step < planes)
        def _():
            relay(step)

        @pl.when(step >= LAG)
        def _():
            finish(step - LAG)

            write_eig(step - LAG)

            @pl.when(step == LAG)
            def _():
                face_copy(0).start()

            @pl.when(step == LAG + 1)
            def _():
                face_copy(1).start()

        @pl.when(step >= LAG + 3)
        def _():
            stencil(step - LAG - 2, None)
            write_res(step - LAG - 2, 0)

        @pl.when(step == LINKS_AT)
        def _():
            face_copy(0).wait_recv()
            face_copy(1).wait_recv()
            links_copy().wait_recv()

        @pl.when((step >= LINKS_AT) & (step < LINKS_AT + slots // BLOCK))
        def _():
            link_block(step - LINKS_AT)

        @pl.when(step == LINKS_AT + slots // BLOCK)
        def _():
            stencil(0, 0)
            write_res(0, 0)

    last = planes - 1
    each(0, last + LAG, advance)
    finish(last)
    for slot in range(3):
        stencil(last - 2 + slot, 1 if slot == 2 else None, slot)

    sums = jnp.sum(stat_out[...].reshape(2 * vector_part, CHUNKS, LANES), axis=1)
    sums = jnp.sum(sums, axis=1, keepdims=True)
    spot = iota((2 * vector_part, LANES), 0) == iota((2 * vector_part, LANES), 1)
    line = jnp.sum(jnp.where(spot, sums, 0.0), axis=0, keepdims=True)
    stat_line[...] = line
    each(0, count - 1, lambda step: stat_copy(1 + (step + 11) % (count - 1)).start())
    write_eig(last)
    for slot in range(3):
        write_res(last - 2 + slot, slot)

    def sent(step):
        first_copy(step).wait_send()
        along_copy(step).wait_send()
        back_copy(step).wait_send()

    each(0, planes, sent)
    links_copy().wait_send()
    face_copy(0).wait_send()
    face_copy(1).wait_send()
    each(1, count, lambda step: stat_copy(step).wait_recv())
    for step in range(1, count):
        line = line + stat_in[step]
    norms = jnp.sqrt(line[:, vector_part : 2 * vector_part]) / jnp.sqrt(line[:, :vector_part] + 1.0)
    norm_out[...] = norms
    each(1, count, lambda step: stat_copy(step).wait_send())


def write_back(eig_held, res_held, norm_held, eig_out, res_out, norm_out, sem):
    copies = [
        pltpu.make_async_copy(source, target, sem.at[place])
        for place, (source, target) in enumerate(
            ((eig_held, eig_out), (res_held, res_out), (norm_held, norm_out))
        )
    ]
    for copy in copies:
        copy.start()
    for copy in copies:
        copy.wait()


def on_device(
    basis,
    coefficients,
    eigen_values,
    stiffness,
    damping,
    mass,
    link_count,
    lower_cells,
    upper_cells,
):
    count = lax.axis_size("rows")
    vector_part = eigen_values.shape[0]
    rank_part, rows_local = basis.shape
    cells = WID * WID
    planes = rows_local // cells
    slots = lower_cells.shape[1]
    held = vector_part * CHUNKS
    width = cells // CHUNKS
    rounds = (count // 2 - 1).bit_length()
    vmem = pl.BlockSpec(memory_space=pltpu.VMEM)
    anywhere = pl.BlockSpec(memory_space=pltpu.HBM)
    dma = pltpu.SemaphoreType.DMA
    wire = pltpu.VMEM((planes, held, width), jnp.bfloat16)
    eigvecs, residuals, norms = pl.pallas_call(
        functools.partial(kernel, count, planes, cells, vector_part, rank_part),
        out_shape=(
            pltpu.VMEM((vector_part, rows_local), jnp.bfloat16),
            pltpu.VMEM((vector_part, rows_local), jnp.bfloat16),
            pltpu.VMEM((1, vector_part), jnp.float32),
        ),
        in_specs=[anywhere] * 9,
        out_specs=(vmem, vmem, vmem),
        scratch_shapes=[
            pltpu.VMEM((planes, rank_part, cells), jnp.bfloat16),
            wire,
            wire,
            wire,
            wire,
            wire,
            wire,
            pltpu.VMEM((planes, held, width), jnp.float32),
            pltpu.VMEM((planes + 2, held, width), jnp.float32),
            wire,
            pltpu.VMEM((3, held, width), jnp.bfloat16),
            pltpu.VMEM((2, held, width), jnp.bfloat16),
            pltpu.VMEM((1, 2 * slots), jnp.int32),
            pltpu.VMEM((1, 2 * slots), jnp.int32),
            pltpu.VMEM((2, width // LANES * held, LANES), jnp.float32),
            pltpu.VMEM((2 * held, LANES), jnp.float32),
            pltpu.VMEM((count, 1, LANES), jnp.float32),
            pltpu.VMEM((1, LANES), jnp.float32),
            pltpu.VMEM((2, 4 * held, CHUNKS * DEPTH), jnp.bfloat16),
            pltpu.VMEM((CHUNKS * PAD, held), jnp.bfloat16),
            pltpu.VMEM((held, held), jnp.bfloat16),
            pltpu.VMEM((3, held, LANES), jnp.float32),
            pltpu.VMEM((rows_local // LANES, LANES), jnp.float32),
            pltpu.VMEM((rows_local // LANES, LANES), jnp.float32),
            pltpu.VMEM((rows_local // LANES, LANES), jnp.float32),
            pltpu.VMEM(coefficients.shape[::-1], jnp.bfloat16),
            pltpu.VMEM((1, vector_part), jnp.float32),
            pltpu.VMEM((1, 1), jnp.int32),
            pltpu.VMEM((1, slots), jnp.int32),
            pltpu.VMEM((1, slots), jnp.int32),
            dma((8,)),
            dma((planes,)),
            dma((planes,)),
            dma((planes,)),
            dma((planes,)),
            dma((planes,)),
            dma((planes,)),
            dma((planes,)),
            dma((3,)),
            dma((3,)),
            dma((count,)),
            dma((count,)),
            pltpu.SemaphoreType.REGULAR((rounds,)),
        ],
        compiler_params=pltpu.CompilerParams(
            collective_id=0, has_side_effects=True, vmem_limit_bytes=56 * 1024 * 1024
        ),
    )(
        basis,
        coefficients.T,
        eigen_values[None, :],
        stiffness.reshape(-1, LANES),
        damping.reshape(-1, LANES),
        mass.reshape(-1, LANES),
        link_count[None, :],
        lower_cells,
        upper_cells,
    )
    eigvecs, residuals, norms = pl.pallas_call(
        write_back,
        out_shape=tuple(
            jax.ShapeDtypeStruct(held.shape, held.dtype) for held in (eigvecs, residuals, norms)
        ),
        in_specs=[vmem] * 3,
        out_specs=[pl.BlockSpec(memory_space=pl.ANY)] * 3,
        scratch_shapes=[dma((3,))],
        compiler_params=pltpu.CompilerParams(vmem_limit_bytes=1 << 20),
    )(eigvecs, residuals, norms)
    return eigvecs, residuals, norms[0]


def solution(mesh):
    placed = (
        P("vecs", "rows"),
        P(),
        P("vecs"),
        P("rows"),
        P("rows"),
        P("rows"),
        P("rows"),
        P("rows", None),
        P("rows", None),
    )
    return jax.shard_map(
        on_device,
        mesh=mesh,
        in_specs=placed,
        out_specs=(P("vecs", "rows"), P("vecs", "rows"), P("vecs")),
        check_vma=False,
    )
```

```python
import functools

import jax
import jax.numpy as jnp
from jax import lax
from jax.experimental import pallas as pl
from jax.experimental.pallas import tpu as pltpu
from jax.sharding import PartitionSpec as P

WID = 64
LANES = 128
CHUNKS = 8
DEPTH = 32
PAD = 16
BLOCK = 512
VECS = 4


def remote(src, dst, send_sem, recv_sem, where):
    return pltpu.make_async_remote_copy(
        src_ref=src,
        dst_ref=dst,
        send_sem=send_sem,
        recv_sem=recv_sem,
        device_id=where,
        device_id_type=pl.DeviceIdType.MESH,
    )


def iota(shape, axis):
    return lax.broadcasted_iota(jnp.int32, shape, axis)


def ones_where(condition):
    return jnp.where(condition, 1.0, 0.0).astype(jnp.bfloat16)


def kernel(
    count,
    planes,
    cells,
    vector_part,
    rank_part,
    basis,
    coefficients_in,
    eigen_in,
    stiffness_in,
    damping_in,
    mass_in,
    used_in,
    lower_in,
    upper_in,
    eig_out,
    res_out,
    norm_out,
    own_basis,
    tail_out,
    raw_in,
    tail_in,
    mid_out,
    mid_in,
    keep,
    last_out,
    last_in,
    values,
    packed,
    res_packed,
    face_in,
    links_in,
    links,
    hot,
    link_sums,
    stat_out,
    stat_in,
    stat_line,
    own_factors,
    mate_factors,
    spread_rows,
    chunk_ones,
    lam_of,
    stiffness,
    damping,
    mass,
    coefficients,
    eigen,
    used,
    lower,
    upper,
    input_sem,
    local_sem,
    raw_send,
    raw_recv,
    mid_send,
    mid_recv,
    last_send,
    last_recv,
    face_send,
    face_recv,
    stat_send,
    stat_recv,
    meet_sem,
):
    row = lax.axis_index("rows")
    vec = lax.axis_index("vecs")
    above = {"rows": (row + 1) % count}
    below = {"rows": (row + count - 1) % count}
    slots = links.shape[1] // 2
    width = cells // CHUNKS
    parts = width // LANES
    held = vector_part * CHUNKS
    plane_rows = cells // LANES
    whole = rank_part // CHUNKS * CHUNKS
    turns = planes // VECS

    def plane_at(step):
        return (step + planes - 1) % planes

    def outer_at(turn, side):
        return turn * VECS + (vec + side) % VECS

    def inner_at(turn, side):
        return turn * VECS + (vec + 3 - side) % VECS

    def inward(side):
        return {"vecs": (vec + 1 + 2 * side) % VECS}

    def outward(side):
        return {"vecs": (vec + 3 - 2 * side) % VECS}

    def local_copy(step):
        start = pl.multiple_of(plane_at(step) * cells, cells)
        return pltpu.make_async_copy(
            basis.at[:, pl.ds(start, cells)],
            own_basis.at[step],
            local_sem.at[step],
        )

    def raw_copy(turn, side, half):
        place = turn * 2 + side
        lanes = pl.ds(half * (cells // 2), cells // 2)
        return remote(
            own_basis.at[outer_at(turn, side), pl.ds(0, whole), lanes],
            raw_in.at[place, :, lanes],
            raw_send.at[half, place],
            raw_recv.at[half, place],
            inward(side),
        )

    def tail_copy(turn, side):
        place = turn * 2 + side
        return remote(
            tail_out.at[place],
            tail_in.at[place],
            raw_send.at[2, place],
            raw_recv.at[2, place],
            inward(side),
        )

    def mid_copy(turn, side):
        place = turn * 2 + side
        other = turn * 2 + 1 - side
        return remote(
            mid_out.at[place],
            mid_in.at[other],
            mid_send.at[place],
            mid_recv.at[other],
            inward(side),
        )

    def last_copy(turn, side):
        place = turn * 2 + side
        return remote(
            last_out.at[place],
            last_in.at[place],
            last_send.at[place],
            last_recv.at[place],
            outward(side),
        )

    def face_copy(which):
        return remote(
            packed.at[which],
            face_in.at[which],
            face_send.at[which],
            face_recv.at[which],
            above if which == 0 else below,
        )

    def links_copy():
        return remote(links, links_in, face_send.at[2], face_recv.at[2], above)

    def stat_copy(step):
        return remote(
            stat_line,
            stat_in.at[step],
            stat_send.at[step],
            stat_recv.at[step],
            {"rows": (row + step) % count},
        )

    def each(first, last, body):
        def run(step, carry):
            body(step)
            return carry

        lax.fori_loop(first, last, run, 0)

    barrier = pltpu.get_barrier_semaphore()

    def greet(where):
        pl.semaphore_signal(barrier, inc=1, device_id=where, device_id_type=pl.DeviceIdType.MESH)

    coefficients_copy = pltpu.make_async_copy(coefficients_in, coefficients, input_sem.at[0])
    coefficients_copy.start()

    def load(turn):
        for side in range(2):
            local_copy(outer_at(turn, side)).start()
        for side in range(2):
            local_copy(inner_at(turn, side)).start()

    each(0, turns, load)
    inputs = [
        pltpu.make_async_copy(source, target, input_sem.at[place + 1])
        for place, (source, target) in enumerate(
            (
                (eigen_in, eigen),
                (used_in, used),
                (lower_in, lower),
                (upper_in, upper),
                (stiffness_in, stiffness),
                (damping_in, damping),
                (mass_in, mass),
            )
        )
    ]
    for copy in inputs:
        copy.start()
    greet({"vecs": (vec + 1) % VECS})
    greet({"vecs": (vec + 3) % VECS})
    greet(above)
    greet(below)

    def meet(round_):
        for where in (row + 2**round_, row + count - 2**round_):
            pl.semaphore_signal(
                meet_sem.at[round_],
                inc=1,
                device_id={"rows": where % count},
                device_id_type=pl.DeviceIdType.MESH,
            )

    unused = jnp.zeros((DEPTH - rank_part, width), jnp.bfloat16)
    deep = CHUNKS * DEPTH
    column = iota((CHUNKS, deep), 1)
    pick_tail = ones_where(column == iota((CHUNKS, deep), 0) * DEPTH + whole)

    def stack_own(step):
        pieces = []
        for chunk in range(CHUNKS):
            pieces += [own_basis[step, :, chunk * width : (chunk + 1) * width], unused]
        return jnp.concatenate(pieces, axis=0)

    def send_half(turn, half):
        def send(side):
            if half == 0:
                local_copy(outer_at(turn, side)).wait()
            raw_copy(turn, side, half).start()

        each(0, 2, send)

    def send_tail(turn):
        def send(side):
            tail = jnp.dot(
                pick_tail, stack_own(outer_at(turn, side)), preferred_element_type=jnp.float32
            )
            tail_out[turn * 2 + side] = tail.astype(jnp.bfloat16)
            tail_copy(turn, side).start()

        each(0, 2, send)

    pl.semaphore_wait(barrier, 4)
    meet(0)
    for turn in range(2):
        send_half(turn, 0)
        send_half(turn, 1)
        send_tail(turn)

    coefficients_copy.wait()
    total_rank, total_vectors = coefficients.shape[1], coefficients.shape[0]
    rank = iota((total_rank, deep), 0)
    column = iota((total_rank, deep), 1)
    own_chunk = column // DEPTH
    own_depth = column & (DEPTH - 1)
    mate_chunk = jnp.zeros_like(column)
    for chunk in range(1, CHUNKS):
        mate_chunk = mate_chunk + (column >= chunk * whole).astype(jnp.int32)
    in_tail = column >= CHUNKS * whole
    mate_depth = jnp.where(in_tail, whole, column - mate_chunk * whole)
    mate_chunk = jnp.where(in_tail, column - CHUNKS * whole, mate_chunk)

    def factor_rows(chunk, depth, source):
        pick = ones_where((rank == source * rank_part + depth) & (depth < rank_part))
        ranks = jnp.dot(coefficients[...], pick, preferred_element_type=jnp.float32)
        ranks = ranks.astype(jnp.bfloat16)
        same_chunk = (iota((held, deep), 0) & (CHUNKS - 1)) == chunk[:held]

        def of_owner(owner):
            choose = ones_where(vector == owner * vector_part + vector_of)
            part = jnp.dot(choose, ranks, preferred_element_type=jnp.float32)
            return jnp.where(same_chunk, part, 0.0).astype(jnp.bfloat16)

        return of_owner

    vector = iota((held, total_vectors), 1)
    vector_of = iota((held, total_vectors), 0) // CHUNKS
    own_of = factor_rows(own_chunk, own_depth, vec)
    mate_of = [
        factor_rows(mate_chunk, mate_depth, (vec + 3 - 2 * side) % VECS) for side in range(2)
    ]
    for place, ahead in enumerate((1, 2, 0, 3)):
        part = own_of((vec + ahead) % VECS)
        own_factors[0, place * held : (place + 1) * held] = part
        other = 3 - place if ahead % 2 else place
        own_factors[1, other * held : (other + 1) * held] = part
        for side in range(2):
            owner = (vec + (ahead if side == 0 else VECS - ahead)) % VECS
            mate_factors[side, place * held : (place + 1) * held] = mate_of[side](owner)

    def inner(turn):
        def run(side):
            place = turn * 2 + side
            step = inner_at(turn, side)
            local_copy(step).wait()
            for half in range(2):
                raw_copy(turn, side, half).wait_recv()
            tail_copy(turn, side).wait_recv()
            own = stack_own(step)
            pieces = [
                raw_in[place, :, chunk * width : (chunk + 1) * width] for chunk in range(CHUNKS)
            ]
            mate = jnp.concatenate([*pieces, tail_in[place]], axis=0)

            def part(rows):
                return jnp.dot(
                    own_factors[side, rows], own, preferred_element_type=jnp.float32
                ) + jnp.dot(
                    mate_factors[side, rows, : CHUNKS * (whole + 1)],
                    mate,
                    preferred_element_type=jnp.float32,
                )

            mid_out[place] = part(slice(0, 2 * held)).astype(jnp.bfloat16)
            mid_copy(turn, side).start()
            keep[place] = part(slice(2 * held, 4 * held))

        each(0, 2, run)

    for copy in inputs:
        copy.wait()
    values[0] = jnp.zeros((held, width), jnp.float32)
    values[planes + 1] = jnp.zeros((held, width), jnp.float32)
    stat_out[...] = jnp.zeros_like(stat_out)
    link_sums[...] = jnp.zeros_like(link_sums)

    is_used = iota((1, slots), 1) < used[...]
    links[:, :slots] = jnp.where(is_used, lower[...], -1)
    links[:, slots:] = jnp.where(is_used, upper[...], -1)
    links_copy().start()

    place = iota((CHUNKS * PAD, held), 0)
    source = iota((CHUNKS * PAD, held), 1)
    spread_rows[...] = ones_where(
        ((place // PAD) == (source & (CHUNKS - 1))) & ((place & (PAD - 1)) == (source // CHUNKS))
    )
    chunk_ones[...] = ones_where(
        (iota((held, held), 0) // CHUNKS) == (iota((held, held), 1) // CHUNKS)
    )
    diag = (iota((held, vector_part), 0) // CHUNKS) == iota((held, vector_part), 1)
    lam = jnp.where(diag, jnp.broadcast_to(eigen[...], (held, vector_part)), 0.0)
    lam = jnp.broadcast_to(jnp.sum(lam, axis=1, keepdims=True), (held, LANES))
    lam_of[0] = lam
    lam_of[1] = lam * lam
    lam_of[2] = lam * lam * 0.1 + lam * 0.3 + 1.0

    def fold(block):
        total = block[:, :LANES]
        for start in range(LANES, block.shape[1], LANES):
            total = total + block[:, start : start + LANES]
        return total

    def write(out, plane, block):
        moved = jnp.dot(spread_rows[...], block, preferred_element_type=jnp.float32)
        for chunk in range(CHUNKS):
            start = pl.multiple_of(plane * cells + chunk * width, width)
            piece = moved[chunk * PAD : (chunk + 1) * PAD].astype(jnp.bfloat16)
            out[:, pl.ds(start, width)] = piece[:vector_part]

    def settle(step, rows, rounded):
        exact = rounded.astype(jnp.float32)
        values[plane_at(step) + 1, rows] = exact
        packed[step, rows] = rounded
        stat_out[rows] += fold(exact * exact)

    def join(turn):
        def run(side):
            place = turn * 2 + side
            mid_copy(turn, 1 - side).wait_recv()

            def total(start):
                rows = slice(start, start + PAD)
                return (keep[place, rows] + mid_in[place, rows].astype(jnp.float32)).astype(
                    jnp.bfloat16
                )

            for start in range(0, held, PAD):
                last_out[place, start : start + PAD] = total(held + start)
            last_copy(turn, side).start()
            step = inner_at(turn, side)
            for start in range(0, held, PAD):
                settle(step, slice(start, start + PAD), total(start))
            write_eig(step)

        each(0, 2, run)

    def close(turn, is_last):
        def run(side):
            place = turn * 2 + side
            last_copy(turn, side).wait_recv()
            step = outer_at(turn, side)
            for start in range(0, held, PAD):
                rows = slice(start, start + PAD)
                settle(step, rows, last_in[place, rows])
            if not is_last:
                write_eig(step)

        each(0, 2, run)

    def write_eig(step):
        write(eig_out, plane_at(step), packed[step])

    def write_res(plane, slot):
        write(res_out, plane, res_packed[slot])

    column = iota((PAD, LANES), 1)
    not_left = (column & (WID - 1)) != 0
    not_right = (column & (WID - 1)) != WID - 1
    low_half = column < WID
    chunk_of = iota((PAD, LANES), 0) & (CHUNKS - 1)
    not_first = chunk_of != 0
    not_last = chunk_of != CHUNKS - 1

    def stencil(plane, link, slot=0):
        diagonals = []
        for part in range(parts):
            at = pl.ds(plane * plane_rows + part, CHUNKS, stride=parts)
            diagonals.append(
                [jnp.concatenate([array[at]] * 2, axis=0) for array in (mass, damping, stiffness)]
            )
        for start in range(0, held, PAD):
            rows = slice(start, start + PAD)
            lam = lam_of[0, rows]
            lam_sq = lam_of[1, rows]
            coupling = lam_of[2, rows]
            mids = [
                values[plane + 1, rows, part * LANES : (part + 1) * LANES] for part in range(parts)
            ]
            swapped = [pltpu.roll(mid, WID, 1) for mid in mids]
            before = jnp.where(not_first, pltpu.roll(swapped[-1], 1, 0), 0.0)
            after = jnp.where(not_last, pltpu.roll(swapped[0], PAD - 1, 0), 0.0)
            swapped = [before, *swapped, after]
            squares = jnp.zeros((PAD, LANES), jnp.float32)
            for part in range(parts):
                lanes = slice(part * LANES, (part + 1) * LANES)
                mid = mids[part]
                total = values[plane, rows, lanes] + values[plane + 2, rows, lanes]
                total = total + (
                    swapped[part + 1] + jnp.where(low_half, swapped[part], swapped[part + 2])
                )
                total = total + jnp.where(not_right, pltpu.roll(mid, LANES - 1, 1), 0.0)
                total = total + jnp.where(not_left, pltpu.roll(mid, 1, 1), 0.0)
                if link is not None:
                    at = part * held + start
                    total = total + link_sums[link, at : at + PAD]
                mass_b, damping_b, stiffness_b = diagonals[part]
                diagonal = lam_sq * mass_b + lam * damping_b + stiffness_b
                full = diagonal * mid - coupling * total
                res_packed[slot, rows, lanes] = full.astype(jnp.bfloat16)
                squares = squares + full * full
            at = slice(held + start, held + start + PAD)
            stat_out[at] += squares

    low_iota = iota((LANES, BLOCK), 0)
    row_chunk = iota((held, BLOCK), 0) & (CHUNKS - 1)

    sides = ((0, links_in, 0, 1), (1, links, 1, 0))

    def make_hot(step):
        start = pl.multiple_of(step * BLOCK, BLOCK)
        for which, lists, *ends in sides:
            for end, end_row in enumerate(ends):
                cell = lists[:, pl.ds(end_row * slots + start, BLOCK)]
                hot[2 * which + end, step] = ones_where(low_iota == (cell & (LANES - 1)))

    def link_block(step):
        start = pl.multiple_of(step * BLOCK, BLOCK)
        targets, picked, got = [], [], []
        for which, lists, source_row, target_row in sides:
            stacked = jnp.concatenate(
                [face_in[which, :, part * LANES : (part + 1) * LANES] for part in range(parts)],
                axis=0,
            )
            source = lists[:, pl.ds(source_row * slots + start, BLOCK)]
            targets.append(lists[:, pl.ds(target_row * slots + start, BLOCK)])
            rows = jnp.dot(stacked, hot[2 * which, step], preferred_element_type=jnp.float32)
            picked.append((source, rows))
        for source, rows in picked:
            high = jnp.broadcast_to(source >> 7, (held, BLOCK))
            total = jnp.zeros((held, BLOCK), jnp.float32)
            for part in range(parts):
                mine = high == row_chunk * parts + part
                total = total + jnp.where(mine, rows[part * held : (part + 1) * held], 0.0)
            got.append(
                jnp.dot(
                    chunk_ones[...], total.astype(jnp.bfloat16), preferred_element_type=jnp.float32
                )
            )
        for (which, *_), target, value in zip(sides, targets, got):
            high = jnp.broadcast_to(target >> 7, (held, BLOCK))
            placed = jnp.concatenate(
                [
                    jnp.where(high == row_chunk * parts + part, value, 0.0).astype(jnp.bfloat16)
                    for part in range(parts)
                ],
                axis=0,
            )
            link_sums[which] += lax.dot_general(
                placed,
                hot[2 * which + 1, step],
                (((1,), (1,)), ((), ())),
                preferred_element_type=jnp.float32,
            )

    rounds = meet_sem.shape[0]

    def met(round_):
        pl.semaphore_wait(meet_sem.at[round_], 2)
        if round_ + 1 < rounds:
            meet(round_ + 1)

    def plain(plane):
        stencil(plane, None)
        write_res(plane, 0)

    blocks = slots // BLOCK

    inner(0)
    send_half(2, 0)
    met(0)
    links_copy().wait_recv()
    each(0, blocks, make_hot)
    join(0)
    send_half(2, 1)
    send_tail(2)
    inner(1)
    met(1)
    close(0, False)
    face_copy(0).start()
    face_copy(1).start()
    send_half(3, 0)
    plain(1)
    met(2)
    face_copy(0).wait_recv()
    face_copy(1).wait_recv()
    each(0, 2, link_block)
    join(1)
    send_half(3, 1)
    send_tail(3)
    inner(2)
    each(2, 3, link_block)
    met(3)
    close(1, False)
    each(2, 6, plain)
    each(3, 4, link_block)
    inner(3)
    each(4, 6, link_block)
    join(2)
    each(6, blocks, link_block)
    stencil(0, 0)
    write_res(0, 0)
    join(3)
    close(2, False)
    each(6, 10, plain)
    close(3, True)
    tail = range(10, planes)
    for slot, plane in enumerate(tail):
        stencil(plane, 1 if plane == planes - 1 else None, slot)

    sums = jnp.sum(stat_out[...].reshape(2 * vector_part, CHUNKS, LANES), axis=1)
    sums = jnp.sum(sums, axis=1, keepdims=True)
    spot = iota((2 * vector_part, LANES), 0) == iota((2 * vector_part, LANES), 1)
    line = jnp.sum(jnp.where(spot, sums, 0.0), axis=0, keepdims=True)
    stat_line[...] = line
    each(0, count - 1, lambda step: stat_copy(1 + (step + 11) % (count - 1)).start())
    each(0, 2, lambda side: write_eig(outer_at(turns - 1, side)))
    for slot, plane in enumerate(tail):
        write_res(plane, slot)

    def sent(turn):
        for side in range(2):
            for half in range(2):
                raw_copy(turn, side, half).wait_send()
            tail_copy(turn, side).wait_send()
            mid_copy(turn, side).wait_send()
            last_copy(turn, side).wait_send()

    each(0, turns, sent)
    links_copy().wait_send()
    face_copy(0).wait_send()
    face_copy(1).wait_send()
    each(1, count, lambda step: stat_copy(step).wait_recv())
    for step in range(1, count):
        line = line + stat_in[step]
    norms = jnp.sqrt(line[:, vector_part : 2 * vector_part]) / jnp.sqrt(line[:, :vector_part] + 1.0)
    norm_out[...] = norms
    each(1, count, lambda step: stat_copy(step).wait_send())


def write_back(eig_held, res_held, norm_held, eig_out, res_out, norm_out, sem):
    copies = [
        pltpu.make_async_copy(source, target, sem.at[place])
        for place, (source, target) in enumerate(
            ((eig_held, eig_out), (res_held, res_out), (norm_held, norm_out))
        )
    ]
    for copy in copies:
        copy.start()
    for copy in copies:
        copy.wait()


def on_device(
    basis,
    coefficients,
    eigen_values,
    stiffness,
    damping,
    mass,
    link_count,
    lower_cells,
    upper_cells,
):
    count = lax.axis_size("rows")
    vector_part = eigen_values.shape[0]
    rank_part, rows_local = basis.shape
    cells = WID * WID
    planes = rows_local // cells
    slots = lower_cells.shape[1]
    held = vector_part * CHUNKS
    width = cells // CHUNKS
    rounds = (count // 2 - 1).bit_length()
    vmem = pl.BlockSpec(memory_space=pltpu.VMEM)
    anywhere = pl.BlockSpec(memory_space=pltpu.HBM)
    dma = pltpu.SemaphoreType.DMA
    pairs = planes // VECS * 2
    whole = rank_part // CHUNKS * CHUNKS

    def wire(*shape):
        return pltpu.VMEM(shape, jnp.bfloat16)

    eigvecs, residuals, norms = pl.pallas_call(
        functools.partial(kernel, count, planes, cells, vector_part, rank_part),
        out_shape=(
            pltpu.VMEM((vector_part, rows_local), jnp.bfloat16),
            pltpu.VMEM((vector_part, rows_local), jnp.bfloat16),
            pltpu.VMEM((1, vector_part), jnp.float32),
        ),
        in_specs=[anywhere] * 9,
        out_specs=(vmem, vmem, vmem),
        scratch_shapes=[
            pltpu.VMEM((planes, rank_part, cells), jnp.bfloat16),
            wire(pairs, CHUNKS, width),
            wire(pairs, whole, cells),
            wire(pairs, CHUNKS, width),
            wire(pairs, 2 * held, width),
            wire(pairs, 2 * held, width),
            pltpu.VMEM((pairs, 2 * held, width), jnp.float32),
            wire(pairs, held, width),
            wire(pairs, held, width),
            pltpu.VMEM((planes + 2, held, width), jnp.float32),
            wire(planes, held, width),
            wire(6, held, width),
            pltpu.VMEM((2, held, width), jnp.bfloat16),
            pltpu.VMEM((1, 2 * slots), jnp.int32),
            pltpu.VMEM((1, 2 * slots), jnp.int32),
            wire(4, slots // BLOCK, LANES, BLOCK),
            pltpu.VMEM((2, width // LANES * held, LANES), jnp.float32),
            pltpu.VMEM((2 * held, LANES), jnp.float32),
            pltpu.VMEM((count, 1, LANES), jnp.float32),
            pltpu.VMEM((1, LANES), jnp.float32),
            wire(2, 4 * held, CHUNKS * DEPTH),
            wire(2, 4 * held, CHUNKS * DEPTH),
            pltpu.VMEM((CHUNKS * PAD, held), jnp.bfloat16),
            pltpu.VMEM((held, held), jnp.bfloat16),
            pltpu.VMEM((3, held, LANES), jnp.float32),
            pltpu.VMEM((rows_local // LANES, LANES), jnp.float32),
            pltpu.VMEM((rows_local // LANES, LANES), jnp.float32),
            pltpu.VMEM((rows_local // LANES, LANES), jnp.float32),
            pltpu.VMEM(coefficients.shape[::-1], jnp.bfloat16),
            pltpu.VMEM((1, vector_part), jnp.float32),
            pltpu.VMEM((1, 1), jnp.int32),
            pltpu.VMEM((1, slots), jnp.int32),
            pltpu.VMEM((1, slots), jnp.int32),
            dma((8,)),
            dma((planes,)),
            dma((3, pairs)),
            dma((3, pairs)),
            dma((pairs,)),
            dma((pairs,)),
            dma((pairs,)),
            dma((pairs,)),
            dma((3,)),
            dma((3,)),
            dma((count,)),
            dma((count,)),
            pltpu.SemaphoreType.REGULAR((rounds,)),
        ],
        compiler_params=pltpu.CompilerParams(
            collective_id=0, has_side_effects=True, vmem_limit_bytes=56 * 1024 * 1024
        ),
    )(
        basis,
        coefficients.T,
        eigen_values[None, :],
        stiffness.reshape(-1, LANES),
        damping.reshape(-1, LANES),
        mass.reshape(-1, LANES),
        link_count[None, :],
        lower_cells,
        upper_cells,
    )
    eigvecs, residuals, norms = pl.pallas_call(
        write_back,
        out_shape=tuple(
            jax.ShapeDtypeStruct(held.shape, held.dtype) for held in (eigvecs, residuals, norms)
        ),
        in_specs=[vmem] * 3,
        out_specs=[pl.BlockSpec(memory_space=pl.ANY)] * 3,
        scratch_shapes=[dma((3,))],
        compiler_params=pltpu.CompilerParams(vmem_limit_bytes=1 << 20),
    )(eigvecs, residuals, norms)
    return eigvecs, residuals, norms[0]


def solution(mesh):
    placed = (
        P("vecs", "rows"),
        P(),
        P("vecs"),
        P("rows"),
        P("rows"),
        P("rows"),
        P("rows"),
        P("rows", None),
        P("rows", None),
    )
    return jax.shard_map(
        on_device,
        mesh=mesh,
        in_specs=placed,
        out_specs=(P("vecs", "rows"), P("vecs", "rows"), P("vecs")),
        check_vma=False,
    )
```

```python
import functools

import jax
import jax.numpy as jnp
from jax import lax
from jax.experimental import pallas as pl
from jax.experimental.pallas import tpu as pltpu
from jax.sharding import PartitionSpec as P

WID = 64
LANES = 128
CHUNKS = 8
DEPTH = 32
PAD = 16
BLOCK = 512
VECS = 4


def remote(src, dst, send_sem, recv_sem, where):
    return pltpu.make_async_remote_copy(
        src_ref=src,
        dst_ref=dst,
        send_sem=send_sem,
        recv_sem=recv_sem,
        device_id=where,
        device_id_type=pl.DeviceIdType.MESH,
    )


def iota(shape, axis):
    return lax.broadcasted_iota(jnp.int32, shape, axis)


def ones_where(condition):
    return jnp.where(condition, 1.0, 0.0).astype(jnp.bfloat16)


def kernel(
    count,
    planes,
    cells,
    vector_part,
    rank_part,
    basis,
    coefficients_in,
    eigen_in,
    stiffness_in,
    damping_in,
    mass_in,
    used_in,
    lower_in,
    upper_in,
    eig_out,
    res_out,
    norm_out,
    own_basis,
    tail_out,
    raw_in,
    tail_in,
    mid_out,
    mid_in,
    keep,
    last_out,
    last_in,
    values,
    packed,
    res_packed,
    face_in,
    links_in,
    links,
    hot,
    link_sums,
    stat_out,
    stat_in,
    stat_line,
    own_factors,
    mate_factors,
    spread_rows,
    chunk_ones,
    lam_of,
    stiffness,
    damping,
    mass,
    coefficients,
    eigen,
    used,
    lower,
    upper,
    input_sem,
    local_sem,
    raw_send,
    raw_recv,
    mid_send,
    mid_recv,
    last_send,
    last_recv,
    face_send,
    face_recv,
    stat_send,
    stat_recv,
    meet_sem,
):
    row = lax.axis_index("rows")
    vec = lax.axis_index("vecs")
    above = {"rows": (row + 1) % count}
    below = {"rows": (row + count - 1) % count}
    slots = links.shape[1] // 2
    width = cells // CHUNKS
    parts = width // LANES
    held = vector_part * CHUNKS
    plane_rows = cells // LANES
    whole = rank_part // CHUNKS * CHUNKS
    turns = planes // VECS
    first = held // 2 // PAD * PAD + PAD
    cuts = ((0, first), (first, held - first))

    def plane_at(step):
        return (step + planes - 1) % planes

    def outer_at(turn, side):
        return turn * VECS + (vec + side) % VECS

    def inner_at(turn, side):
        return turn * VECS + (vec + 3 - side) % VECS

    def inward(side):
        return {"vecs": (vec + 1 + 2 * side) % VECS}

    def outward(side):
        return {"vecs": (vec + 3 - 2 * side) % VECS}

    def local_copy(step):
        start = pl.multiple_of(plane_at(step) * cells, cells)
        return pltpu.make_async_copy(
            basis.at[:, pl.ds(start, cells)],
            own_basis.at[step],
            local_sem.at[step],
        )

    def raw_copy(turn, side, half):
        place = turn * 2 + side
        lanes = pl.ds(half * (cells // 2), cells // 2)
        return remote(
            own_basis.at[outer_at(turn, side), pl.ds(0, whole), lanes],
            raw_in.at[place, :, lanes],
            raw_send.at[half, place],
            raw_recv.at[half, place],
            inward(side),
        )

    def tail_copy(turn, side):
        place = turn * 2 + side
        return remote(
            tail_out.at[place],
            tail_in.at[place],
            raw_send.at[2, place],
            raw_recv.at[2, place],
            inward(side),
        )

    def mid_copy(turn, side, half):
        place = turn * 2 + side
        other = turn * 2 + 1 - side
        rows = pl.ds((1 - half) * held, held)
        return remote(
            mid_out.at[place, rows],
            mid_in.at[other, rows],
            mid_send.at[half, place],
            mid_recv.at[half, other],
            inward(side),
        )

    def last_copy(turn, side, half):
        place = turn * 2 + side
        rows = pl.ds(*cuts[half])
        return remote(
            last_out.at[place, rows],
            last_in.at[place, rows],
            last_send.at[half, place],
            last_recv.at[half, place],
            outward(side),
        )

    def face_copy(which):
        return remote(
            packed.at[which],
            face_in.at[which],
            face_send.at[which],
            face_recv.at[which],
            above if which == 0 else below,
        )

    def links_copy():
        return remote(links, links_in, face_send.at[2], face_recv.at[2], above)

    def stat_copy(step):
        return remote(
            stat_line,
            stat_in.at[step],
            stat_send.at[0],
            stat_recv.at[0],
            {"rows": (row + step) % count},
        )

    def all_stats():
        lines = stat_in.at[pl.ds(1, count - 1)]
        return remote(lines, lines, stat_send.at[0], stat_recv.at[0], above)

    def each(begin, end, body):
        def run(step, carry):
            body(step)
            return carry

        lax.fori_loop(begin, end, run, 0)

    barrier = pltpu.get_barrier_semaphore()

    def greet(where):
        pl.semaphore_signal(barrier, inc=1, device_id=where, device_id_type=pl.DeviceIdType.MESH)

    greet({"vecs": (vec + 1) % VECS})
    greet({"vecs": (vec + 3) % VECS})
    greet(above)
    greet(below)

    coefficients_copy = pltpu.make_async_copy(coefficients_in, coefficients, input_sem.at[0])
    coefficients_copy.start()

    def load(turn):
        for side in range(2):
            local_copy(outer_at(turn, side)).start()
        for side in range(2):
            local_copy(inner_at(turn, side)).start()

    each(0, turns, load)
    inputs = [
        pltpu.make_async_copy(source, target, input_sem.at[place + 1])
        for place, (source, target) in enumerate(
            (
                (eigen_in, eigen),
                (used_in, used),
                (lower_in, lower),
                (upper_in, upper),
                (stiffness_in, stiffness),
                (damping_in, damping),
                (mass_in, mass),
            )
        )
    ]
    for copy in inputs:
        copy.start()

    def meet(round_):
        for where in (row + 2**round_, row + count - 2**round_):
            pl.semaphore_signal(
                meet_sem.at[round_],
                inc=1,
                device_id={"rows": where % count},
                device_id_type=pl.DeviceIdType.MESH,
            )

    unused = jnp.zeros((DEPTH - rank_part, width), jnp.bfloat16)
    deep = CHUNKS * DEPTH
    column = iota((CHUNKS, deep), 1)
    pick_tail = ones_where(column == iota((CHUNKS, deep), 0) * DEPTH + whole)

    def stack_own(step):
        pieces = []
        for chunk in range(CHUNKS):
            pieces += [own_basis[step, :, chunk * width : (chunk + 1) * width], unused]
        return jnp.concatenate(pieces, axis=0)

    def send_half(turn, half):
        def send(side):
            if half == 0:
                local_copy(outer_at(turn, side)).wait()
            raw_copy(turn, side, half).start()

        each(0, 2, send)

    def send_tail(turn):
        def send(side):
            tail = jnp.dot(
                pick_tail, stack_own(outer_at(turn, side)), preferred_element_type=jnp.float32
            )
            tail_out[turn * 2 + side] = tail.astype(jnp.bfloat16)
            tail_copy(turn, side).start()

        each(0, 2, send)

    pl.semaphore_wait(barrier, 4)
    meet(0)
    for turn in range(2):
        send_half(turn, 0)
        send_half(turn, 1)
        send_tail(turn)

    coefficients_copy.wait()
    total_rank, total_vectors = coefficients.shape[1], coefficients.shape[0]
    rank = iota((total_rank, deep), 0)
    column = iota((total_rank, deep), 1)
    own_chunk = column // DEPTH
    own_depth = column & (DEPTH - 1)
    mate_chunk = jnp.zeros_like(column)
    for chunk in range(1, CHUNKS):
        mate_chunk = mate_chunk + (column >= chunk * whole).astype(jnp.int32)
    in_tail = column >= CHUNKS * whole
    mate_depth = jnp.where(in_tail, whole, column - mate_chunk * whole)
    mate_chunk = jnp.where(in_tail, column - CHUNKS * whole, mate_chunk)

    def factor_rows(chunk, depth, source):
        pick = ones_where((rank == source * rank_part + depth) & (depth < rank_part))
        ranks = jnp.dot(coefficients[...], pick, preferred_element_type=jnp.float32)
        ranks = ranks.astype(jnp.bfloat16)
        same_chunk = (iota((held, deep), 0) & (CHUNKS - 1)) == chunk[:held]

        def of_owner(owner):
            choose = ones_where(vector == owner * vector_part + vector_of)
            part = jnp.dot(choose, ranks, preferred_element_type=jnp.float32)
            return jnp.where(same_chunk, part, 0.0).astype(jnp.bfloat16)

        return of_owner

    vector = iota((held, total_vectors), 1)
    vector_of = iota((held, total_vectors), 0) // CHUNKS
    own_of = factor_rows(own_chunk, own_depth, vec)
    mate_of = [
        factor_rows(mate_chunk, mate_depth, (vec + 3 - 2 * side) % VECS) for side in range(2)
    ]
    for place, ahead in enumerate((1, 2, 0, 3)):
        part = own_of((vec + ahead) % VECS)
        own_factors[0, place * held : (place + 1) * held] = part
        other = 3 - place if ahead % 2 else place
        own_factors[1, other * held : (other + 1) * held] = part
        for side in range(2):
            owner = (vec + (ahead if side == 0 else VECS - ahead)) % VECS
            mate_factors[side, place * held : (place + 1) * held] = mate_of[side](owner)

    def inner(turn):
        def run(side):
            place = turn * 2 + side
            step = inner_at(turn, side)
            local_copy(step).wait()
            for half in range(2):
                raw_copy(turn, side, half).wait_recv()
            tail_copy(turn, side).wait_recv()
            own = stack_own(step)
            pieces = [
                raw_in[place, :, chunk * width : (chunk + 1) * width] for chunk in range(CHUNKS)
            ]
            mate = jnp.concatenate([*pieces, tail_in[place]], axis=0)

            def part(rows):
                return jnp.dot(
                    own_factors[side, rows], own, preferred_element_type=jnp.float32
                ) + jnp.dot(
                    mate_factors[side, rows, : CHUNKS * (whole + 1)],
                    mate,
                    preferred_element_type=jnp.float32,
                )

            mid_out[place] = part(slice(0, 2 * held)).astype(jnp.bfloat16)
            mid_copy(turn, side, 0).start()
            mid_copy(turn, side, 1).start()
            keep[place] = part(slice(2 * held, 4 * held))

        each(0, 2, run)

    for copy in inputs:
        copy.wait()
    values[0] = jnp.zeros((held, width), jnp.float32)
    values[planes + 1] = jnp.zeros((held, width), jnp.float32)
    stat_out[...] = jnp.zeros_like(stat_out)
    link_sums[...] = jnp.zeros_like(link_sums)

    is_used = iota((1, slots), 1) < used[...]
    links[:, :slots] = jnp.where(is_used, lower[...], -1)
    links[:, slots:] = jnp.where(is_used, upper[...], -1)
    links_copy().start()

    place = iota((CHUNKS * PAD, held), 0)
    source = iota((CHUNKS * PAD, held), 1)
    spread_rows[...] = ones_where(
        ((place // PAD) == (source & (CHUNKS - 1))) & ((place & (PAD - 1)) == (source // CHUNKS))
    )
    chunk_ones[...] = ones_where(
        (iota((held, held), 0) // CHUNKS) == (iota((held, held), 1) // CHUNKS)
    )
    diag = (iota((held, vector_part), 0) // CHUNKS) == iota((held, vector_part), 1)
    lam = jnp.where(diag, jnp.broadcast_to(eigen[...], (held, vector_part)), 0.0)
    lam = jnp.broadcast_to(jnp.sum(lam, axis=1, keepdims=True), (held, LANES))
    lam_of[0] = lam
    lam_of[1] = lam * lam
    lam_of[2] = lam * lam * 0.1 + lam * 0.3 + 1.0

    def fold(block):
        total = block[:, :LANES]
        for start in range(LANES, block.shape[1], LANES):
            total = total + block[:, start : start + LANES]
        return total

    def write(out, plane, block):
        moved = jnp.dot(spread_rows[...], block, preferred_element_type=jnp.float32)
        for chunk in range(CHUNKS):
            start = pl.multiple_of(plane * cells + chunk * width, width)
            piece = moved[chunk * PAD : (chunk + 1) * PAD].astype(jnp.bfloat16)
            out[:, pl.ds(start, width)] = piece[:vector_part]

    def settle(step, rows, rounded):
        exact = rounded.astype(jnp.float32)
        values[plane_at(step) + 1, rows] = exact
        packed[step, rows] = rounded
        stat_out[rows] += fold(exact * exact)

    def join(turn):
        def total(place, start):
            rows = slice(start, start + PAD)
            return (keep[place, rows] + mid_in[place, rows].astype(jnp.float32)).astype(
                jnp.bfloat16
            )

        def send(side):
            place = turn * 2 + side
            mid_copy(turn, 1 - side, 0).wait_recv()
            for half, (start, size) in enumerate(cuts):
                for at in range(start, start + size, PAD):
                    last_out[place, at : at + PAD] = total(place, held + at)
                last_copy(turn, side, half).start()

        def own(side):
            place = turn * 2 + side
            mid_copy(turn, 1 - side, 1).wait_recv()
            step = inner_at(turn, side)
            for start in range(0, held, PAD):
                settle(step, slice(start, start + PAD), total(place, start))
            write_eig(step)

        each(0, 2, send)
        each(0, 2, own)

    def close_part(turn, side, half):
        last_copy(turn, side, half).wait_recv()
        start, size = cuts[half]
        for at in range(start, start + size, PAD):
            rows = slice(at, at + PAD)
            settle(outer_at(turn, side), rows, last_in[turn * 2 + side, rows])

    def close(turn):
        def run(side):
            close_part(turn, side, 0)
            close_part(turn, side, 1)
            write_eig(outer_at(turn, side))

        each(0, 2, run)

    def write_eig(step):
        write(eig_out, plane_at(step), packed[step])

    def write_res(plane, slot):
        write(res_out, plane, res_packed[slot])

    column = iota((PAD, LANES), 1)
    not_left = (column & (WID - 1)) != 0
    not_right = (column & (WID - 1)) != WID - 1
    low_half = column < WID
    chunk_of = iota((PAD, LANES), 0) & (CHUNKS - 1)
    not_first = chunk_of != 0
    not_last = chunk_of != CHUNKS - 1

    def stencil(plane, link, slot=0, begin=0, size=held):
        diagonals = []
        for part in range(parts):
            at = pl.ds(plane * plane_rows + part, CHUNKS, stride=parts)
            diagonals.append(
                [jnp.concatenate([array[at]] * 2, axis=0) for array in (mass, damping, stiffness)]
            )
        for start in range(begin, begin + size, PAD):
            rows = slice(start, start + PAD)
            lam = lam_of[0, rows]
            lam_sq = lam_of[1, rows]
            coupling = lam_of[2, rows]
            mids = [
                values[plane + 1, rows, part * LANES : (part + 1) * LANES] for part in range(parts)
            ]
            swapped = [pltpu.roll(mid, WID, 1) for mid in mids]
            before = jnp.where(not_first, pltpu.roll(swapped[-1], 1, 0), 0.0)
            after = jnp.where(not_last, pltpu.roll(swapped[0], PAD - 1, 0), 0.0)
            swapped = [before, *swapped, after]
            squares = jnp.zeros((PAD, LANES), jnp.float32)
            for part in range(parts):
                lanes = slice(part * LANES, (part + 1) * LANES)
                mid = mids[part]
                total = values[plane, rows, lanes] + values[plane + 2, rows, lanes]
                total = total + (
                    swapped[part + 1] + jnp.where(low_half, swapped[part], swapped[part + 2])
                )
                total = total + jnp.where(not_right, pltpu.roll(mid, LANES - 1, 1), 0.0)
                total = total + jnp.where(not_left, pltpu.roll(mid, 1, 1), 0.0)
                if link is not None:
                    at = part * held + start
                    total = total + link_sums[link, at : at + PAD]
                mass_b, damping_b, stiffness_b = diagonals[part]
                diagonal = lam_sq * mass_b + lam * damping_b + stiffness_b
                full = diagonal * mid - coupling * total
                res_packed[slot, rows, lanes] = full.astype(jnp.bfloat16)
                squares = squares + full * full
            at = slice(held + start, held + start + PAD)
            stat_out[at] += squares

    low_iota = iota((LANES, BLOCK), 0)
    row_chunk = iota((held, BLOCK), 0) & (CHUNKS - 1)

    sides = ((0, links_in, 0, 1), (1, links, 1, 0))

    def make_hot(step):
        start = pl.multiple_of(step * BLOCK, BLOCK)
        for which, lists, *ends in sides:
            for end, end_row in enumerate(ends):
                cell = lists[:, pl.ds(end_row * slots + start, BLOCK)]
                hot[2 * which + end, step] = ones_where(low_iota == (cell & (LANES - 1)))

    def link_block(step):
        start = pl.multiple_of(step * BLOCK, BLOCK)
        targets, picked, got = [], [], []
        for which, lists, source_row, target_row in sides:
            stacked = jnp.concatenate(
                [face_in[which, :, part * LANES : (part + 1) * LANES] for part in range(parts)],
                axis=0,
            )
            source = lists[:, pl.ds(source_row * slots + start, BLOCK)]
            targets.append(lists[:, pl.ds(target_row * slots + start, BLOCK)])
            rows = jnp.dot(stacked, hot[2 * which, step], preferred_element_type=jnp.float32)
            picked.append((source, rows))
        for source, rows in picked:
            high = jnp.broadcast_to(source >> 7, (held, BLOCK))
            total = jnp.zeros((held, BLOCK), jnp.float32)
            for part in range(parts):
                mine = high == row_chunk * parts + part
                total = total + jnp.where(mine, rows[part * held : (part + 1) * held], 0.0)
            got.append(
                jnp.dot(
                    chunk_ones[...], total.astype(jnp.bfloat16), preferred_element_type=jnp.float32
                )
            )
        for (which, *_), target, value in zip(sides, targets, got):
            high = jnp.broadcast_to(target >> 7, (held, BLOCK))
            placed = jnp.concatenate(
                [
                    jnp.where(high == row_chunk * parts + part, value, 0.0).astype(jnp.bfloat16)
                    for part in range(parts)
                ],
                axis=0,
            )
            link_sums[which] += lax.dot_general(
                placed,
                hot[2 * which + 1, step],
                (((1,), (1,)), ((), ())),
                preferred_element_type=jnp.float32,
            )

    rounds = meet_sem.shape[0]

    def met(round_):
        pl.semaphore_wait(meet_sem.at[round_], 2)
        if round_ + 1 < rounds:
            meet(round_ + 1)

    def plain(plane):
        stencil(plane, None)
        write_res(plane, 0)

    blocks = slots // BLOCK

    inner(0)
    send_half(2, 0)
    met(0)
    links_copy().wait_recv()
    each(0, blocks, make_hot)
    join(0)
    send_half(2, 1)
    send_tail(2)
    inner(1)
    met(1)
    close(0)
    face_copy(0).start()
    face_copy(1).start()
    send_half(3, 0)
    plain(1)
    met(2)
    face_copy(0).wait_recv()
    face_copy(1).wait_recv()
    each(0, 2, link_block)
    join(1)
    send_half(3, 1)
    send_tail(3)
    inner(2)
    each(2, 3, link_block)
    met(3)
    close(1)
    each(2, 6, plain)
    each(3, 4, link_block)
    inner(3)
    each(4, 6, link_block)
    join(2)
    each(6, blocks, link_block)
    stencil(0, 0)
    write_res(0, 0)
    join(3)
    close(2)
    each(6, 10, plain)
    tail = range(10, planes)
    for half in range(2):
        each(0, 2, lambda side: close_part(3, side, half))
        for slot, plane in enumerate(tail):
            stencil(plane, 1 if plane == planes - 1 else None, slot, *cuts[half])

    sums = jnp.sum(stat_out[...].reshape(2 * vector_part, CHUNKS, LANES), axis=1)
    sums = jnp.sum(sums, axis=1, keepdims=True)
    spot = iota((2 * vector_part, LANES), 0) == iota((2 * vector_part, LANES), 1)
    line = jnp.sum(jnp.where(spot, sums, 0.0), axis=0, keepdims=True)
    stat_line[...] = line
    far = count // 3
    each(far, count, lambda step: stat_copy(step).start())
    each(1, far, lambda step: stat_copy(step).start())
    each(0, 2, lambda side: write_eig(outer_at(turns - 1, side)))
    for slot, plane in enumerate(tail):
        write_res(plane, slot)

    def sent(turn):
        for side in range(2):
            for half in range(2):
                raw_copy(turn, side, half).wait_send()
            tail_copy(turn, side).wait_send()
            for half in range(2):
                mid_copy(turn, side, half).wait_send()
                last_copy(turn, side, half).wait_send()

    each(0, turns, sent)
    links_copy().wait_send()
    face_copy(0).wait_send()
    face_copy(1).wait_send()
    all_stats().wait_recv()
    for step in range(1, count):
        line = line + stat_in[step]
    norms = jnp.sqrt(line[:, vector_part : 2 * vector_part]) / jnp.sqrt(line[:, :vector_part] + 1.0)
    norm_out[...] = norms
    all_stats().wait_send()


def write_back(eig_held, res_held, norm_held, eig_out, res_out, norm_out, sem):
    copies = [
        pltpu.make_async_copy(source, target, sem.at[place])
        for place, (source, target) in enumerate(
            ((eig_held, eig_out), (res_held, res_out), (norm_held, norm_out))
        )
    ]
    for copy in copies:
        copy.start()
    for copy in copies:
        copy.wait()


def on_device(
    basis,
    coefficients,
    eigen_values,
    stiffness,
    damping,
    mass,
    link_count,
    lower_cells,
    upper_cells,
):
    count = lax.axis_size("rows")
    vector_part = eigen_values.shape[0]
    rank_part, rows_local = basis.shape
    cells = WID * WID
    planes = rows_local // cells
    slots = lower_cells.shape[1]
    held = vector_part * CHUNKS
    width = cells // CHUNKS
    rounds = (count // 2 - 1).bit_length()
    vmem = pl.BlockSpec(memory_space=pltpu.VMEM)
    anywhere = pl.BlockSpec(memory_space=pltpu.HBM)
    dma = pltpu.SemaphoreType.DMA
    pairs = planes // VECS * 2
    whole = rank_part // CHUNKS * CHUNKS

    def wire(*shape):
        return pltpu.VMEM(shape, jnp.bfloat16)

    eigvecs, residuals, norms = pl.pallas_call(
        functools.partial(kernel, count, planes, cells, vector_part, rank_part),
        out_shape=(
            pltpu.VMEM((vector_part, rows_local), jnp.bfloat16),
            pltpu.VMEM((vector_part, rows_local), jnp.bfloat16),
            pltpu.VMEM((1, vector_part), jnp.float32),
        ),
        in_specs=[anywhere] * 9,
        out_specs=(vmem, vmem, vmem),
        scratch_shapes=[
            pltpu.VMEM((planes, rank_part, cells), jnp.bfloat16),
            wire(pairs, CHUNKS, width),
            wire(pairs, whole, cells),
            wire(pairs, CHUNKS, width),
            wire(pairs, 2 * held, width),
            wire(pairs, 2 * held, width),
            pltpu.VMEM((pairs, 2 * held, width), jnp.float32),
            wire(pairs, held, width),
            wire(pairs, held, width),
            pltpu.VMEM((planes + 2, held, width), jnp.float32),
            wire(planes, held, width),
            wire(6, held, width),
            pltpu.VMEM((2, held, width), jnp.bfloat16),
            pltpu.VMEM((1, 2 * slots), jnp.int32),
            pltpu.VMEM((1, 2 * slots), jnp.int32),
            wire(4, slots // BLOCK, LANES, BLOCK),
            pltpu.VMEM((2, width // LANES * held, LANES), jnp.float32),
            pltpu.VMEM((2 * held, LANES), jnp.float32),
            pltpu.VMEM((count, 1, LANES), jnp.float32),
            pltpu.VMEM((1, LANES), jnp.float32),
            wire(2, 4 * held, CHUNKS * DEPTH),
            wire(2, 4 * held, CHUNKS * DEPTH),
            pltpu.VMEM((CHUNKS * PAD, held), jnp.bfloat16),
            pltpu.VMEM((held, held), jnp.bfloat16),
            pltpu.VMEM((3, held, LANES), jnp.float32),
            pltpu.VMEM((rows_local // LANES, LANES), jnp.float32),
            pltpu.VMEM((rows_local // LANES, LANES), jnp.float32),
            pltpu.VMEM((rows_local // LANES, LANES), jnp.float32),
            pltpu.VMEM(coefficients.shape[::-1], jnp.bfloat16),
            pltpu.VMEM((1, vector_part), jnp.float32),
            pltpu.VMEM((1, 1), jnp.int32),
            pltpu.VMEM((1, slots), jnp.int32),
            pltpu.VMEM((1, slots), jnp.int32),
            dma((8,)),
            dma((planes,)),
            dma((3, pairs)),
            dma((3, pairs)),
            dma((2, pairs)),
            dma((2, pairs)),
            dma((2, pairs)),
            dma((2, pairs)),
            dma((3,)),
            dma((3,)),
            dma((1,)),
            dma((1,)),
            pltpu.SemaphoreType.REGULAR((rounds,)),
        ],
        compiler_params=pltpu.CompilerParams(
            collective_id=0, has_side_effects=True, vmem_limit_bytes=56 * 1024 * 1024
        ),
    )(
        basis,
        coefficients.T,
        eigen_values[None, :],
        stiffness.reshape(-1, LANES),
        damping.reshape(-1, LANES),
        mass.reshape(-1, LANES),
        link_count[None, :],
        lower_cells,
        upper_cells,
    )
    eigvecs, residuals, norms = pl.pallas_call(
        write_back,
        out_shape=tuple(
            jax.ShapeDtypeStruct(held.shape, held.dtype) for held in (eigvecs, residuals, norms)
        ),
        in_specs=[vmem] * 3,
        out_specs=[pl.BlockSpec(memory_space=pl.ANY)] * 3,
        scratch_shapes=[dma((3,))],
        compiler_params=pltpu.CompilerParams(vmem_limit_bytes=1 << 20),
    )(eigvecs, residuals, norms)
    return eigvecs, residuals, norms[0]


def solution(mesh):
    placed = (
        P("vecs", "rows"),
        P(),
        P("vecs"),
        P("rows"),
        P("rows"),
        P("rows"),
        P("rows"),
        P("rows", None),
        P("rows", None),
    )
    return jax.shard_map(
        on_device,
        mesh=mesh,
        in_specs=placed,
        out_specs=(P("vecs", "rows"), P("vecs", "rows"), P("vecs")),
        check_vma=False,
    )
```

```python
import functools

import jax
import jax.numpy as jnp
from jax import lax
from jax.experimental import pallas as pl
from jax.experimental.pallas import tpu as pltpu
from jax.sharding import PartitionSpec as P

WID = 64
LANES = 128
CHUNKS = 8
DEPTH = 32
PAD = 16
BLOCK = 512
VECS = 4


def remote(src, dst, send_sem, recv_sem, where):
    return pltpu.make_async_remote_copy(
        src_ref=src,
        dst_ref=dst,
        send_sem=send_sem,
        recv_sem=recv_sem,
        device_id=where,
        device_id_type=pl.DeviceIdType.MESH,
    )


def iota(shape, axis):
    return lax.broadcasted_iota(jnp.int32, shape, axis)


def ones_where(condition):
    return jnp.where(condition, 1.0, 0.0).astype(jnp.bfloat16)


def kernel(
    count,
    planes,
    cells,
    vector_part,
    rank_part,
    basis,
    coefficients_in,
    eigen_in,
    stiffness_in,
    damping_in,
    mass_in,
    used_in,
    lower_in,
    upper_in,
    eig_out,
    res_out,
    norm_out,
    own_basis,
    tail_out,
    raw_in,
    tail_in,
    mid_out,
    mid_in,
    keep,
    last_out,
    last_in,
    values,
    packed,
    res_packed,
    face_in,
    links_in,
    links,
    hot,
    link_sums,
    stat_out,
    stat_in,
    stat_line,
    own_factors,
    mate_factors,
    spread_rows,
    chunk_ones,
    lam_of,
    stiffness,
    damping,
    mass,
    coefficients,
    eigen,
    used,
    lower,
    upper,
    input_sem,
    local_sem,
    raw_send,
    raw_recv,
    mid_send,
    mid_recv,
    last_send,
    last_recv,
    face_send,
    face_recv,
    stat_send,
    stat_recv,
    meet_sem,
):
    row = lax.axis_index("rows")
    vec = lax.axis_index("vecs")
    above = {"rows": (row + 1) % count}
    below = {"rows": (row + count - 1) % count}
    slots = links.shape[1] // 2
    width = cells // CHUNKS
    parts = width // LANES
    held = vector_part * CHUNKS
    plane_rows = cells // LANES
    whole = rank_part // CHUNKS * CHUNKS
    turns = planes // VECS
    first = held // 2 // PAD * PAD + PAD
    cuts = ((0, first), (first, held - first))

    def plane_at(step):
        return (step + planes - 1) % planes

    def outer_at(turn, side):
        return turn * VECS + (vec + side) % VECS

    def inner_at(turn, side):
        return turn * VECS + (vec + 3 - side) % VECS

    def inward(side):
        return {"vecs": (vec + 1 + 2 * side) % VECS}

    def outward(side):
        return {"vecs": (vec + 3 - 2 * side) % VECS}

    def local_copy(step):
        start = pl.multiple_of(plane_at(step) * cells, cells)
        return pltpu.make_async_copy(
            basis.at[:, pl.ds(start, cells)],
            own_basis.at[step],
            local_sem.at[step],
        )

    def raw_copy(turn, side, half):
        place = turn * 2 + side
        lanes = pl.ds(half * (cells // 2), cells // 2)
        return remote(
            own_basis.at[outer_at(turn, side), pl.ds(0, whole), lanes],
            raw_in.at[place, :, lanes],
            raw_send.at[half, place],
            raw_recv.at[half, place],
            inward(side),
        )

    def tail_copy(turn, side):
        place = turn * 2 + side
        return remote(
            tail_out.at[place],
            tail_in.at[place],
            raw_send.at[2, place],
            raw_recv.at[2, place],
            inward(side),
        )

    def mid_copy(turn, side, half):
        place = turn * 2 + side
        other = turn * 2 + 1 - side
        rows = pl.ds((1 - half) * held, held)
        return remote(
            mid_out.at[place, rows],
            mid_in.at[other, rows],
            mid_send.at[half, place],
            mid_recv.at[half, other],
            inward(side),
        )

    def last_copy(turn, side, half):
        place = turn * 2 + side
        rows = pl.ds(*cuts[half])
        return remote(
            last_out.at[place, rows],
            last_in.at[place, rows],
            last_send.at[half, place],
            last_recv.at[half, place],
            outward(side),
        )

    def face_copy(which):
        return remote(
            packed.at[which],
            face_in.at[which],
            face_send.at[which],
            face_recv.at[which],
            above if which == 0 else below,
        )

    def links_copy():
        return remote(links, links_in, face_send.at[2], face_recv.at[2], above)

    def stat_copy(step):
        return remote(
            stat_line,
            stat_in.at[step],
            stat_send.at[0],
            stat_recv.at[0],
            {"rows": (row + step) % count},
        )

    def distance(step):
        across, along = step // 8, step // 2 % 4
        return -min(across, 4 - across) - min(along, 4 - along)

    def all_stats():
        lines = stat_in.at[pl.ds(1, count - 1)]
        return remote(lines, lines, stat_send.at[0], stat_recv.at[0], above)

    def each(begin, end, body):
        def run(step, carry):
            body(step)
            return carry

        lax.fori_loop(begin, end, run, 0)

    barrier = pltpu.get_barrier_semaphore()

    def greet(where):
        pl.semaphore_signal(barrier, inc=1, device_id=where, device_id_type=pl.DeviceIdType.MESH)

    greet({"vecs": (vec + 1) % VECS})
    greet({"vecs": (vec + 3) % VECS})
    greet(above)
    greet(below)

    coefficients_copy = pltpu.make_async_copy(coefficients_in, coefficients, input_sem.at[0])
    coefficients_copy.start()

    def load(turn):
        for side in range(2):
            local_copy(outer_at(turn, side)).start()
        for side in range(2):
            local_copy(inner_at(turn, side)).start()

    each(0, turns, load)
    inputs = [
        pltpu.make_async_copy(source, target, input_sem.at[place + 1])
        for place, (source, target) in enumerate(
            (
                (eigen_in, eigen),
                (used_in, used),
                (lower_in, lower),
                (upper_in, upper),
                (stiffness_in, stiffness),
                (damping_in, damping),
                (mass_in, mass),
            )
        )
    ]
    for copy in inputs:
        copy.start()

    def meet(round_):
        for where in (row + 2**round_, row + count - 2**round_):
            pl.semaphore_signal(
                meet_sem.at[round_],
                inc=1,
                device_id={"rows": where % count},
                device_id_type=pl.DeviceIdType.MESH,
            )

    unused = jnp.zeros((DEPTH - rank_part, width), jnp.bfloat16)
    deep = CHUNKS * DEPTH
    column = iota((CHUNKS, deep), 1)
    pick_tail = ones_where(column == iota((CHUNKS, deep), 0) * DEPTH + whole)

    def stack_own(step):
        pieces = []
        for chunk in range(CHUNKS):
            pieces += [own_basis[step, :, chunk * width : (chunk + 1) * width], unused]
        return jnp.concatenate(pieces, axis=0)

    def send_half(turn, half):
        def send(side):
            if half == 0:
                local_copy(outer_at(turn, side)).wait()
            raw_copy(turn, side, half).start()

        each(0, 2, send)

    def send_tail(turn):
        def send(side):
            tail = jnp.dot(
                pick_tail, stack_own(outer_at(turn, side)), preferred_element_type=jnp.float32
            )
            tail_out[turn * 2 + side] = tail.astype(jnp.bfloat16)
            tail_copy(turn, side).start()

        each(0, 2, send)

    pl.semaphore_wait(barrier, 4)
    meet(0)
    for turn in range(2):
        send_half(turn, 0)
        send_half(turn, 1)
        send_tail(turn)

    coefficients_copy.wait()
    total_rank, total_vectors = coefficients.shape[1], coefficients.shape[0]
    rank = iota((total_rank, deep), 0)
    column = iota((total_rank, deep), 1)
    own_chunk = column // DEPTH
    own_depth = column & (DEPTH - 1)
    mate_chunk = jnp.zeros_like(column)
    for chunk in range(1, CHUNKS):
        mate_chunk = mate_chunk + (column >= chunk * whole).astype(jnp.int32)
    in_tail = column >= CHUNKS * whole
    mate_depth = jnp.where(in_tail, whole, column - mate_chunk * whole)
    mate_chunk = jnp.where(in_tail, column - CHUNKS * whole, mate_chunk)

    def factor_rows(chunk, depth, source):
        pick = ones_where((rank == source * rank_part + depth) & (depth < rank_part))
        ranks = jnp.dot(coefficients[...], pick, preferred_element_type=jnp.float32)
        ranks = ranks.astype(jnp.bfloat16)
        same_chunk = (iota((held, deep), 0) & (CHUNKS - 1)) == chunk[:held]

        def of_owner(owner):
            choose = ones_where(vector == owner * vector_part + vector_of)
            part = jnp.dot(choose, ranks, preferred_element_type=jnp.float32)
            return jnp.where(same_chunk, part, 0.0).astype(jnp.bfloat16)

        return of_owner

    vector = iota((held, total_vectors), 1)
    vector_of = iota((held, total_vectors), 0) // CHUNKS
    own_of = factor_rows(own_chunk, own_depth, vec)
    mate_of = [
        factor_rows(mate_chunk, mate_depth, (vec + 3 - 2 * side) % VECS) for side in range(2)
    ]
    for place, ahead in enumerate((1, 2, 0, 3)):
        part = own_of((vec + ahead) % VECS)
        own_factors[0, place * held : (place + 1) * held] = part
        other = 3 - place if ahead % 2 else place
        own_factors[1, other * held : (other + 1) * held] = part
        for side in range(2):
            owner = (vec + (ahead if side == 0 else VECS - ahead)) % VECS
            mate_factors[side, place * held : (place + 1) * held] = mate_of[side](owner)

    def inner(turn):
        def run(side):
            place = turn * 2 + side
            step = inner_at(turn, side)
            local_copy(step).wait()
            for half in range(2):
                raw_copy(turn, side, half).wait_recv()
            tail_copy(turn, side).wait_recv()
            own = stack_own(step)
            pieces = [
                raw_in[place, :, chunk * width : (chunk + 1) * width] for chunk in range(CHUNKS)
            ]
            mate = jnp.concatenate([*pieces, tail_in[place]], axis=0)

            def part(rows):
                return jnp.dot(
                    own_factors[side, rows], own, preferred_element_type=jnp.float32
                ) + jnp.dot(
                    mate_factors[side, rows, : CHUNKS * (whole + 1)],
                    mate,
                    preferred_element_type=jnp.float32,
                )

            mid_out[place] = part(slice(0, 2 * held)).astype(jnp.bfloat16)
            mid_copy(turn, side, 0).start()
            mid_copy(turn, side, 1).start()
            keep[place] = part(slice(2 * held, 4 * held))

        each(0, 2, run)

    for copy in inputs:
        copy.wait()
    values[0] = jnp.zeros((held, width), jnp.float32)
    values[planes + 1] = jnp.zeros((held, width), jnp.float32)
    stat_out[...] = jnp.zeros_like(stat_out)
    link_sums[...] = jnp.zeros_like(link_sums)

    is_used = iota((1, slots), 1) < used[...]
    links[:, :slots] = jnp.where(is_used, lower[...], -1)
    links[:, slots:] = jnp.where(is_used, upper[...], -1)
    links_copy().start()

    place = iota((CHUNKS * PAD, held), 0)
    source = iota((CHUNKS * PAD, held), 1)
    spread_rows[...] = ones_where(
        ((place // PAD) == (source & (CHUNKS - 1))) & ((place & (PAD - 1)) == (source // CHUNKS))
    )
    chunk_ones[...] = ones_where(
        (iota((held, held), 0) // CHUNKS) == (iota((held, held), 1) // CHUNKS)
    )
    diag = (iota((held, vector_part), 0) // CHUNKS) == iota((held, vector_part), 1)
    lam = jnp.where(diag, jnp.broadcast_to(eigen[...], (held, vector_part)), 0.0)
    lam = jnp.broadcast_to(jnp.sum(lam, axis=1, keepdims=True), (held, LANES))
    lam_of[0] = lam
    lam_of[1] = lam * lam
    lam_of[2] = lam * lam * 0.1 + lam * 0.3 + 1.0

    def fold(block):
        total = block[:, :LANES]
        for start in range(LANES, block.shape[1], LANES):
            total = total + block[:, start : start + LANES]
        return total

    def write(out, plane, block):
        moved = jnp.dot(spread_rows[...], block, preferred_element_type=jnp.float32)
        for chunk in range(CHUNKS):
            start = pl.multiple_of(plane * cells + chunk * width, width)
            piece = moved[chunk * PAD : (chunk + 1) * PAD].astype(jnp.bfloat16)
            out[:, pl.ds(start, width)] = piece[:vector_part]

    def settle(step, rows, rounded):
        exact = rounded.astype(jnp.float32)
        values[plane_at(step) + 1, rows] = exact
        packed[step, rows] = rounded
        stat_out[rows] += fold(exact * exact)

    def join(turn, late=False):
        def total(place, start):
            rows = slice(start, start + PAD)
            return (keep[place, rows] + mid_in[place, rows].astype(jnp.float32)).astype(
                jnp.bfloat16
            )

        def send(side):
            place = turn * 2 + side
            mid_copy(turn, 1 - side, 0).wait_recv()
            for half, (start, size) in enumerate(cuts):
                for at in range(start, start + size, PAD):
                    last_out[place, at : at + PAD] = total(place, held + at)
                last_copy(turn, side, half).start()

        def own(side):
            place = turn * 2 + side
            mid_copy(turn, 1 - side, 1).wait_recv()
            step = inner_at(turn, side)
            for start in range(0, held, PAD):
                settle(step, slice(start, start + PAD), total(place, start))
            if not late:
                write_eig(step)

        each(0, 2, send)
        each(0, 2, own)

    def close_part(turn, side, half):
        last_copy(turn, side, half).wait_recv()
        start, size = cuts[half]
        for at in range(start, start + size, PAD):
            rows = slice(at, at + PAD)
            settle(outer_at(turn, side), rows, last_in[turn * 2 + side, rows])

    def close(turn, late=False):
        def run(side):
            close_part(turn, side, 0)
            close_part(turn, side, 1)
            if not late:
                write_eig(outer_at(turn, side))

        each(0, 2, run)

    def write_eig(step):
        write(eig_out, plane_at(step), packed[step])

    def write_res(plane, slot):
        write(res_out, plane, res_packed[slot])

    column = iota((PAD, LANES), 1)
    not_left = (column & (WID - 1)) != 0
    not_right = (column & (WID - 1)) != WID - 1
    low_half = column < WID
    chunk_of = iota((PAD, LANES), 0) & (CHUNKS - 1)
    not_first = chunk_of != 0
    not_last = chunk_of != CHUNKS - 1

    def stencil(plane, link, slot=0, begin=0, size=held):
        diagonals = []
        for part in range(parts):
            at = pl.ds(plane * plane_rows + part, CHUNKS, stride=parts)
            diagonals.append(
                [jnp.concatenate([array[at]] * 2, axis=0) for array in (mass, damping, stiffness)]
            )
        for start in range(begin, begin + size, PAD):
            rows = slice(start, start + PAD)
            lam = lam_of[0, rows]
            lam_sq = lam_of[1, rows]
            coupling = lam_of[2, rows]
            mids = [
                values[plane + 1, rows, part * LANES : (part + 1) * LANES] for part in range(parts)
            ]
            swapped = [pltpu.roll(mid, WID, 1) for mid in mids]
            before = jnp.where(not_first, pltpu.roll(swapped[-1], 1, 0), 0.0)
            after = jnp.where(not_last, pltpu.roll(swapped[0], PAD - 1, 0), 0.0)
            swapped = [before, *swapped, after]
            squares = jnp.zeros((PAD, LANES), jnp.float32)
            for part in range(parts):
                lanes = slice(part * LANES, (part + 1) * LANES)
                mid = mids[part]
                total = values[plane, rows, lanes] + values[plane + 2, rows, lanes]
                total = total + (
                    swapped[part + 1] + jnp.where(low_half, swapped[part], swapped[part + 2])
                )
                total = total + jnp.where(not_right, pltpu.roll(mid, LANES - 1, 1), 0.0)
                total = total + jnp.where(not_left, pltpu.roll(mid, 1, 1), 0.0)
                if link is not None:
                    at = part * held + start
                    total = total + link_sums[link, at : at + PAD]
                mass_b, damping_b, stiffness_b = diagonals[part]
                diagonal = lam_sq * mass_b + lam * damping_b + stiffness_b
                full = diagonal * mid - coupling * total
                res_packed[slot, rows, lanes] = full.astype(jnp.bfloat16)
                squares = squares + full * full
            at = slice(held + start, held + start + PAD)
            stat_out[at] += squares

    low_iota = iota((LANES, BLOCK), 0)
    row_chunk = iota((held, BLOCK), 0) & (CHUNKS - 1)

    sides = ((0, links_in, 0, 1), (1, links, 1, 0))

    def make_hot(step):
        start = pl.multiple_of(step * BLOCK, BLOCK)
        for which, lists, *ends in sides:
            for end, end_row in enumerate(ends):
                cell = lists[:, pl.ds(end_row * slots + start, BLOCK)]
                hot[2 * which + end, step] = ones_where(low_iota == (cell & (LANES - 1)))

    def link_block(step):
        start = pl.multiple_of(step * BLOCK, BLOCK)
        targets, picked, got = [], [], []
        for which, lists, source_row, target_row in sides:
            stacked = jnp.concatenate(
                [face_in[which, :, part * LANES : (part + 1) * LANES] for part in range(parts)],
                axis=0,
            )
            source = lists[:, pl.ds(source_row * slots + start, BLOCK)]
            targets.append(lists[:, pl.ds(target_row * slots + start, BLOCK)])
            rows = jnp.dot(stacked, hot[2 * which, step], preferred_element_type=jnp.float32)
            picked.append((source, rows))
        for source, rows in picked:
            high = jnp.broadcast_to(source >> 7, (held, BLOCK))
            total = jnp.zeros((held, BLOCK), jnp.float32)
            for part in range(parts):
                mine = high == row_chunk * parts + part
                total = total + jnp.where(mine, rows[part * held : (part + 1) * held], 0.0)
            got.append(
                jnp.dot(
                    chunk_ones[...], total.astype(jnp.bfloat16), preferred_element_type=jnp.float32
                )
            )
        for (which, *_), target, value in zip(sides, targets, got):
            high = jnp.broadcast_to(target >> 7, (held, BLOCK))
            placed = jnp.concatenate(
                [
                    jnp.where(high == row_chunk * parts + part, value, 0.0).astype(jnp.bfloat16)
                    for part in range(parts)
                ],
                axis=0,
            )
            link_sums[which] += lax.dot_general(
                placed,
                hot[2 * which + 1, step],
                (((1,), (1,)), ((), ())),
                preferred_element_type=jnp.float32,
            )

    rounds = meet_sem.shape[0]

    def met(round_):
        pl.semaphore_wait(meet_sem.at[round_], 2)
        if round_ + 1 < rounds:
            meet(round_ + 1)

    def plain(plane):
        stencil(plane, None)
        write_res(plane, 0)

    blocks = slots // BLOCK

    inner(0)
    send_half(2, 0)
    met(0)
    links_copy().wait_recv()
    each(0, blocks, make_hot)
    join(0)
    send_half(2, 1)
    send_tail(2)
    inner(1)
    met(1)
    close(0)
    face_copy(0).start()
    face_copy(1).start()
    send_half(3, 0)
    plain(1)
    met(2)
    face_copy(0).wait_recv()
    face_copy(1).wait_recv()
    each(0, 2, link_block)
    join(1)
    send_half(3, 1)
    send_tail(3)
    inner(2)
    each(2, 3, link_block)
    met(3)
    close(1)
    each(2, 6, plain)
    each(3, 5, link_block)
    inner(3)
    each(5, blocks, link_block)
    join(2)
    stencil(0, 0)
    write_res(0, 0)
    join(3, True)
    close(2, True)
    late = 6
    each(late, 10, lambda plane: stencil(plane, None, plane - late))
    tail = range(10, planes)
    for half in range(2):
        each(0, 2, lambda side: close_part(3, side, half))
        for plane in tail:
            stencil(plane, 1 if plane == planes - 1 else None, plane - late, *cuts[half])

    sums = jnp.sum(stat_out[...].reshape(2 * vector_part, CHUNKS, LANES), axis=1)
    sums = jnp.sum(sums, axis=1, keepdims=True)
    spot = iota((2 * vector_part, LANES), 0) == iota((2 * vector_part, LANES), 1)
    line = jnp.sum(jnp.where(spot, sums, 0.0), axis=0, keepdims=True)
    stat_line[...] = line
    for step in sorted(range(1, count), key=distance):
        stat_copy(step).start()
    def write_late(side):
        write_eig(outer_at(2, side))
        write_eig(inner_at(3, side))
        write_eig(outer_at(3, side))

    each(0, 2, write_late)
    each(late, planes, lambda plane: write_res(plane, plane - late))

    def sent(turn):
        for side in range(2):
            for half in range(2):
                raw_copy(turn, side, half).wait_send()
            tail_copy(turn, side).wait_send()
            for half in range(2):
                mid_copy(turn, side, half).wait_send()
                last_copy(turn, side, half).wait_send()

    each(0, turns, sent)
    links_copy().wait_send()
    face_copy(0).wait_send()
    face_copy(1).wait_send()
    all_stats().wait_recv()
    for step in range(1, count):
        line = line + stat_in[step]
    norms = jnp.sqrt(line[:, vector_part : 2 * vector_part]) / jnp.sqrt(line[:, :vector_part] + 1.0)
    norm_out[...] = norms
    all_stats().wait_send()


def write_back(eig_held, res_held, norm_held, eig_out, res_out, norm_out, sem):
    copies = [
        pltpu.make_async_copy(source, target, sem.at[place])
        for place, (source, target) in enumerate(
            ((eig_held, eig_out), (res_held, res_out), (norm_held, norm_out))
        )
    ]
    for copy in copies:
        copy.start()
    for copy in copies:
        copy.wait()


def on_device(
    basis,
    coefficients,
    eigen_values,
    stiffness,
    damping,
    mass,
    link_count,
    lower_cells,
    upper_cells,
):
    count = lax.axis_size("rows")
    vector_part = eigen_values.shape[0]
    rank_part, rows_local = basis.shape
    cells = WID * WID
    planes = rows_local // cells
    slots = lower_cells.shape[1]
    held = vector_part * CHUNKS
    width = cells // CHUNKS
    rounds = (count // 2 - 1).bit_length()
    vmem = pl.BlockSpec(memory_space=pltpu.VMEM)
    anywhere = pl.BlockSpec(memory_space=pltpu.HBM)
    dma = pltpu.SemaphoreType.DMA
    pairs = planes // VECS * 2
    whole = rank_part // CHUNKS * CHUNKS

    def wire(*shape):
        return pltpu.VMEM(shape, jnp.bfloat16)

    eigvecs, residuals, norms = pl.pallas_call(
        functools.partial(kernel, count, planes, cells, vector_part, rank_part),
        out_shape=(
            pltpu.VMEM((vector_part, rows_local), jnp.bfloat16),
            pltpu.VMEM((vector_part, rows_local), jnp.bfloat16),
            pltpu.VMEM((1, vector_part), jnp.float32),
        ),
        in_specs=[anywhere] * 9,
        out_specs=(vmem, vmem, vmem),
        scratch_shapes=[
            pltpu.VMEM((planes, rank_part, cells), jnp.bfloat16),
            wire(pairs, CHUNKS, width),
            wire(pairs, whole, cells),
            wire(pairs, CHUNKS, width),
            wire(pairs, 2 * held, width),
            wire(pairs, 2 * held, width),
            pltpu.VMEM((pairs, 2 * held, width), jnp.float32),
            wire(pairs, held, width),
            wire(pairs, held, width),
            pltpu.VMEM((planes + 2, held, width), jnp.float32),
            wire(planes, held, width),
            wire(10, held, width),
            pltpu.VMEM((2, held, width), jnp.bfloat16),
            pltpu.VMEM((1, 2 * slots), jnp.int32),
            pltpu.VMEM((1, 2 * slots), jnp.int32),
            wire(4, slots // BLOCK, LANES, BLOCK),
            pltpu.VMEM((2, width // LANES * held, LANES), jnp.float32),
            pltpu.VMEM((2 * held, LANES), jnp.float32),
            pltpu.VMEM((count, 1, LANES), jnp.float32),
            pltpu.VMEM((1, LANES), jnp.float32),
            wire(2, 4 * held, CHUNKS * DEPTH),
            wire(2, 4 * held, CHUNKS * DEPTH),
            pltpu.VMEM((CHUNKS * PAD, held), jnp.bfloat16),
            pltpu.VMEM((held, held), jnp.bfloat16),
            pltpu.VMEM((3, held, LANES), jnp.float32),
            pltpu.VMEM((rows_local // LANES, LANES), jnp.float32),
            pltpu.VMEM((rows_local // LANES, LANES), jnp.float32),
            pltpu.VMEM((rows_local // LANES, LANES), jnp.float32),
            pltpu.VMEM(coefficients.shape[::-1], jnp.bfloat16),
            pltpu.VMEM((1, vector_part), jnp.float32),
            pltpu.VMEM((1, 1), jnp.int32),
            pltpu.VMEM((1, slots), jnp.int32),
            pltpu.VMEM((1, slots), jnp.int32),
            dma((8,)),
            dma((planes,)),
            dma((3, pairs)),
            dma((3, pairs)),
            dma((2, pairs)),
            dma((2, pairs)),
            dma((2, pairs)),
            dma((2, pairs)),
            dma((3,)),
            dma((3,)),
            dma((1,)),
            dma((1,)),
            pltpu.SemaphoreType.REGULAR((rounds,)),
        ],
        compiler_params=pltpu.CompilerParams(
            collective_id=0, has_side_effects=True, vmem_limit_bytes=56 * 1024 * 1024
        ),
    )(
        basis,
        coefficients.T,
        eigen_values[None, :],
        stiffness.reshape(-1, LANES),
        damping.reshape(-1, LANES),
        mass.reshape(-1, LANES),
        link_count[None, :],
        lower_cells,
        upper_cells,
    )
    eigvecs, residuals, norms = pl.pallas_call(
        write_back,
        out_shape=tuple(
            jax.ShapeDtypeStruct(held.shape, held.dtype) for held in (eigvecs, residuals, norms)
        ),
        in_specs=[vmem] * 3,
        out_specs=[pl.BlockSpec(memory_space=pl.ANY)] * 3,
        scratch_shapes=[dma((3,))],
        compiler_params=pltpu.CompilerParams(vmem_limit_bytes=1 << 20),
    )(eigvecs, residuals, norms)
    return eigvecs, residuals, norms[0]


def solution(mesh):
    placed = (
        P("vecs", "rows"),
        P(),
        P("vecs"),
        P("rows"),
        P("rows"),
        P("rows"),
        P("rows"),
        P("rows", None),
        P("rows", None),
    )
    return jax.shard_map(
        on_device,
        mesh=mesh,
        in_specs=placed,
        out_specs=(P("vecs", "rows"), P("vecs", "rows"), P("vecs")),
        check_vma=False,
    )
```

```python
import functools

import jax
import jax.numpy as jnp
from jax import lax
from jax.experimental import pallas as pl
from jax.experimental.pallas import tpu as pltpu
from jax.sharding import PartitionSpec as P

WID = 64
LANES = 128
CHUNKS = 8
DEPTH = 32
PAD = 16
BLOCK = 512
VECS = 4


def remote(src, dst, send_sem, recv_sem, where):
    return pltpu.make_async_remote_copy(
        src_ref=src,
        dst_ref=dst,
        send_sem=send_sem,
        recv_sem=recv_sem,
        device_id=where,
        device_id_type=pl.DeviceIdType.MESH,
    )


def iota(shape, axis):
    return lax.broadcasted_iota(jnp.int32, shape, axis)


def ones_where(condition):
    return jnp.where(condition, 1.0, 0.0).astype(jnp.bfloat16)


def kernel(
    count,
    planes,
    cells,
    vector_part,
    rank_part,
    basis,
    coefficients_in,
    eigen_in,
    stiffness_in,
    damping_in,
    mass_in,
    used_in,
    lower_in,
    upper_in,
    eig_out,
    res_out,
    norm_out,
    own_basis,
    tail_out,
    raw_in,
    tail_in,
    mid_out,
    mid_in,
    keep,
    last_out,
    last_in,
    values,
    packed,
    res_packed,
    face_in,
    links_in,
    links,
    hot,
    link_sums,
    stat_out,
    stat_in,
    stat_line,
    own_factors,
    mate_factors,
    spread_rows,
    chunk_ones,
    lam_of,
    stiffness,
    damping,
    mass,
    coefficients,
    eigen,
    used,
    lower,
    upper,
    input_sem,
    local_sem,
    raw_send,
    raw_recv,
    mid_send,
    mid_recv,
    last_send,
    last_recv,
    face_send,
    face_recv,
    stat_send,
    stat_recv,
    meet_sem,
):
    row = lax.axis_index("rows")
    vec = lax.axis_index("vecs")
    above = {"rows": (row + 1) % count}
    below = {"rows": (row + count - 1) % count}
    slots = links.shape[1] // 2
    width = cells // CHUNKS
    parts = width // LANES
    held = vector_part * CHUNKS
    plane_rows = cells // LANES
    whole = rank_part // CHUNKS * CHUNKS
    turns = planes // VECS
    first = held // 2 // PAD * PAD + PAD
    cuts = ((0, first), (first, held - first))

    def plane_at(step):
        return (step + planes - 1) % planes

    def outer_at(turn, side):
        return turn * VECS + (vec + side) % VECS

    def inner_at(turn, side):
        return turn * VECS + (vec + 3 - side) % VECS

    def inward(side):
        return {"vecs": (vec + 1 + 2 * side) % VECS}

    def outward(side):
        return {"vecs": (vec + 3 - 2 * side) % VECS}

    def local_copy(step):
        start = pl.multiple_of(plane_at(step) * cells, cells)
        return pltpu.make_async_copy(
            basis.at[:, pl.ds(start, cells)],
            own_basis.at[step],
            local_sem.at[step],
        )

    def raw_copy(turn, side, half):
        place = turn * 2 + side
        early = cells // 8 * 5
        lanes = pl.ds(half * early, cells - early if half else early)
        return remote(
            own_basis.at[outer_at(turn, side), pl.ds(0, whole), lanes],
            raw_in.at[place, :, lanes],
            raw_send.at[half, place],
            raw_recv.at[half, place],
            inward(side),
        )

    def tail_copy(turn, side):
        place = turn * 2 + side
        return remote(
            tail_out.at[place],
            tail_in.at[place],
            raw_send.at[2, place],
            raw_recv.at[2, place],
            inward(side),
        )

    def mid_copy(turn, side, half):
        place = turn * 2 + side
        other = turn * 2 + 1 - side
        rows = pl.ds((1 - half) * held, held)
        return remote(
            mid_out.at[place, rows],
            mid_in.at[other, rows],
            mid_send.at[half, place],
            mid_recv.at[half, other],
            inward(side),
        )

    def last_copy(turn, side, half):
        place = turn * 2 + side
        rows = pl.ds(*cuts[half])
        return remote(
            last_out.at[place, rows],
            last_in.at[place, rows],
            last_send.at[half, place],
            last_recv.at[half, place],
            outward(side),
        )

    def face_copy(which):
        return remote(
            packed.at[which],
            face_in.at[which],
            face_send.at[which],
            face_recv.at[which],
            above if which == 0 else below,
        )

    def links_copy():
        return remote(links, links_in, face_send.at[2], face_recv.at[2], above)

    def stat_copy(step):
        return remote(
            stat_line,
            stat_in.at[step],
            stat_send.at[0],
            stat_recv.at[0],
            {"rows": (row + step) % count},
        )

    def distance(step):
        across, along = step // 8, step // 2 % 4
        return -min(across, 4 - across) - min(along, 4 - along)

    def all_stats():
        lines = stat_in.at[pl.ds(1, count - 1)]
        return remote(lines, lines, stat_send.at[0], stat_recv.at[0], above)

    def each(begin, end, body):
        def run(step, carry):
            body(step)
            return carry

        lax.fori_loop(begin, end, run, 0)

    barrier = pltpu.get_barrier_semaphore()

    def greet(where):
        pl.semaphore_signal(barrier, inc=1, device_id=where, device_id_type=pl.DeviceIdType.MESH)

    greet({"vecs": (vec + 1) % VECS})
    greet({"vecs": (vec + 3) % VECS})
    greet(above)
    greet(below)

    coefficients_copy = pltpu.make_async_copy(coefficients_in, coefficients, input_sem.at[0])
    coefficients_copy.start()

    def load(turn):
        for side in range(2):
            local_copy(outer_at(turn, side)).start()
        for side in range(2):
            local_copy(inner_at(turn, side)).start()

    each(0, turns, load)
    inputs = [
        pltpu.make_async_copy(source, target, input_sem.at[place + 1])
        for place, (source, target) in enumerate(
            (
                (eigen_in, eigen),
                (used_in, used),
                (lower_in, lower),
                (upper_in, upper),
                (stiffness_in, stiffness),
                (damping_in, damping),
                (mass_in, mass),
            )
        )
    ]
    for copy in inputs:
        copy.start()

    def meet(round_):
        for where in (row + 2**round_, row + count - 2**round_):
            pl.semaphore_signal(
                meet_sem.at[round_],
                inc=1,
                device_id={"rows": where % count},
                device_id_type=pl.DeviceIdType.MESH,
            )

    unused = jnp.zeros((DEPTH - rank_part, width), jnp.bfloat16)
    deep = CHUNKS * DEPTH
    column = iota((CHUNKS, deep), 1)
    pick_tail = ones_where(column == iota((CHUNKS, deep), 0) * DEPTH + whole)

    def stack_own(step):
        pieces = []
        for chunk in range(CHUNKS):
            pieces += [own_basis[step, :, chunk * width : (chunk + 1) * width], unused]
        return jnp.concatenate(pieces, axis=0)

    def send_half(turn, half):
        def send(side):
            if half == 0:
                local_copy(outer_at(turn, side)).wait()
            raw_copy(turn, side, half).start()

        each(0, 2, send)

    def send_tail(turn):
        def send(side):
            tail = jnp.dot(
                pick_tail, stack_own(outer_at(turn, side)), preferred_element_type=jnp.float32
            )
            tail_out[turn * 2 + side] = tail.astype(jnp.bfloat16)
            tail_copy(turn, side).start()

        each(0, 2, send)

    pl.semaphore_wait(barrier, 4)
    meet(0)
    for turn in range(2):
        send_half(turn, 0)
        send_half(turn, 1)
        send_tail(turn)

    coefficients_copy.wait()
    total_rank, total_vectors = coefficients.shape[1], coefficients.shape[0]
    rank = iota((total_rank, deep), 0)
    column = iota((total_rank, deep), 1)
    own_chunk = column // DEPTH
    own_depth = column & (DEPTH - 1)
    mate_chunk = jnp.zeros_like(column)
    for chunk in range(1, CHUNKS):
        mate_chunk = mate_chunk + (column >= chunk * whole).astype(jnp.int32)
    in_tail = column >= CHUNKS * whole
    mate_depth = jnp.where(in_tail, whole, column - mate_chunk * whole)
    mate_chunk = jnp.where(in_tail, column - CHUNKS * whole, mate_chunk)

    def factor_rows(chunk, depth, source):
        pick = ones_where((rank == source * rank_part + depth) & (depth < rank_part))
        ranks = jnp.dot(coefficients[...], pick, preferred_element_type=jnp.float32)
        ranks = ranks.astype(jnp.bfloat16)
        same_chunk = (iota((held, deep), 0) & (CHUNKS - 1)) == chunk[:held]

        def of_owner(owner):
            choose = ones_where(vector == owner * vector_part + vector_of)
            part = jnp.dot(choose, ranks, preferred_element_type=jnp.float32)
            return jnp.where(same_chunk, part, 0.0).astype(jnp.bfloat16)

        return of_owner

    vector = iota((held, total_vectors), 1)
    vector_of = iota((held, total_vectors), 0) // CHUNKS
    own_of = factor_rows(own_chunk, own_depth, vec)
    mate_of = [
        factor_rows(mate_chunk, mate_depth, (vec + 3 - 2 * side) % VECS) for side in range(2)
    ]
    for place, ahead in enumerate((1, 2, 0, 3)):
        part = own_of((vec + ahead) % VECS)
        own_factors[0, place * held : (place + 1) * held] = part
        other = 3 - place if ahead % 2 else place
        own_factors[1, other * held : (other + 1) * held] = part
        for side in range(2):
            owner = (vec + (ahead if side == 0 else VECS - ahead)) % VECS
            mate_factors[side, place * held : (place + 1) * held] = mate_of[side](owner)

    def inner(turn):
        def run(side):
            place = turn * 2 + side
            step = inner_at(turn, side)
            local_copy(step).wait()
            for half in range(2):
                raw_copy(turn, side, half).wait_recv()
            tail_copy(turn, side).wait_recv()
            own = stack_own(step)
            pieces = [
                raw_in[place, :, chunk * width : (chunk + 1) * width] for chunk in range(CHUNKS)
            ]
            mate = jnp.concatenate([*pieces, tail_in[place]], axis=0)

            def part(rows):
                return jnp.dot(
                    own_factors[side, rows], own, preferred_element_type=jnp.float32
                ) + jnp.dot(
                    mate_factors[side, rows, : CHUNKS * (whole + 1)],
                    mate,
                    preferred_element_type=jnp.float32,
                )

            mid_out[place] = part(slice(0, 2 * held)).astype(jnp.bfloat16)
            mid_copy(turn, side, 0).start()
            mid_copy(turn, side, 1).start()
            keep[place] = part(slice(2 * held, 4 * held))

        each(0, 2, run)

    for copy in inputs:
        copy.wait()
    values[0] = jnp.zeros((held, width), jnp.float32)
    values[planes + 1] = jnp.zeros((held, width), jnp.float32)
    stat_out[...] = jnp.zeros_like(stat_out)
    link_sums[...] = jnp.zeros_like(link_sums)

    is_used = iota((1, slots), 1) < used[...]
    links[:, :slots] = jnp.where(is_used, lower[...], -1)
    links[:, slots:] = jnp.where(is_used, upper[...], -1)
    links_copy().start()

    place = iota((CHUNKS * PAD, held), 0)
    source = iota((CHUNKS * PAD, held), 1)
    spread_rows[...] = ones_where(
        ((place // PAD) == (source & (CHUNKS - 1))) & ((place & (PAD - 1)) == (source // CHUNKS))
    )
    chunk_ones[...] = ones_where(
        (iota((held, held), 0) // CHUNKS) == (iota((held, held), 1) // CHUNKS)
    )
    diag = (iota((held, vector_part), 0) // CHUNKS) == iota((held, vector_part), 1)
    lam = jnp.where(diag, jnp.broadcast_to(eigen[...], (held, vector_part)), 0.0)
    lam = jnp.broadcast_to(jnp.sum(lam, axis=1, keepdims=True), (held, LANES))
    lam_of[0] = lam
    lam_of[1] = lam * lam
    lam_of[2] = lam * lam * 0.1 + lam * 0.3 + 1.0

    def fold(block):
        total = block[:, :LANES]
        for start in range(LANES, block.shape[1], LANES):
            total = total + block[:, start : start + LANES]
        return total

    def write(out, plane, block):
        moved = jnp.dot(spread_rows[...], block, preferred_element_type=jnp.float32)
        for chunk in range(CHUNKS):
            start = pl.multiple_of(plane * cells + chunk * width, width)
            piece = moved[chunk * PAD : (chunk + 1) * PAD].astype(jnp.bfloat16)
            out[:, pl.ds(start, width)] = piece[:vector_part]

    def settle(step, rows, rounded):
        exact = rounded.astype(jnp.float32)
        values[plane_at(step) + 1, rows] = exact
        packed[step, rows] = rounded
        stat_out[rows] += fold(exact * exact)

    def join(turn, late=False):
        def total(place, start):
            rows = slice(start, start + PAD)
            return (keep[place, rows] + mid_in[place, rows].astype(jnp.float32)).astype(
                jnp.bfloat16
            )

        def send(side):
            place = turn * 2 + side
            mid_copy(turn, 1 - side, 0).wait_recv()
            for half, (start, size) in enumerate(cuts):
                for at in range(start, start + size, PAD):
                    last_out[place, at : at + PAD] = total(place, held + at)
                last_copy(turn, side, half).start()

        def own(side):
            place = turn * 2 + side
            mid_copy(turn, 1 - side, 1).wait_recv()
            step = inner_at(turn, side)
            for start in range(0, held, PAD):
                settle(step, slice(start, start + PAD), total(place, start))
            if not late:
                write_eig(step)

        each(0, 2, send)
        each(0, 2, own)

    def close_part(turn, side, half):
        last_copy(turn, side, half).wait_recv()
        start, size = cuts[half]
        for at in range(start, start + size, PAD):
            rows = slice(at, at + PAD)
            settle(outer_at(turn, side), rows, last_in[turn * 2 + side, rows])

    def close(turn, late=False):
        def run(side):
            close_part(turn, side, 0)
            close_part(turn, side, 1)
            if not late:
                write_eig(outer_at(turn, side))

        each(0, 2, run)

    def write_eig(step):
        write(eig_out, plane_at(step), packed[step])

    def write_res(plane, slot):
        write(res_out, plane, res_packed[slot])

    column = iota((PAD, LANES), 1)
    not_left = (column & (WID - 1)) != 0
    not_right = (column & (WID - 1)) != WID - 1
    low_half = column < WID
    chunk_of = iota((PAD, LANES), 0) & (CHUNKS - 1)
    not_first = chunk_of != 0
    not_last = chunk_of != CHUNKS - 1

    def stencil(plane, link, slot=0, begin=0, size=held):
        diagonals = []
        for part in range(parts):
            at = pl.ds(plane * plane_rows + part, CHUNKS, stride=parts)
            diagonals.append(
                [jnp.concatenate([array[at]] * 2, axis=0) for array in (mass, damping, stiffness)]
            )
        for start in range(begin, begin + size, PAD):
            rows = slice(start, start + PAD)
            lam = lam_of[0, rows]
            lam_sq = lam_of[1, rows]
            coupling = lam_of[2, rows]
            mids = [
                values[plane + 1, rows, part * LANES : (part + 1) * LANES] for part in range(parts)
            ]
            swapped = [pltpu.roll(mid, WID, 1) for mid in mids]
            before = jnp.where(not_first, pltpu.roll(swapped[-1], 1, 0), 0.0)
            after = jnp.where(not_last, pltpu.roll(swapped[0], PAD - 1, 0), 0.0)
            swapped = [before, *swapped, after]
            squares = jnp.zeros((PAD, LANES), jnp.float32)
            for part in range(parts):
                lanes = slice(part * LANES, (part + 1) * LANES)
                mid = mids[part]
                total = values[plane, rows, lanes] + values[plane + 2, rows, lanes]
                total = total + (
                    swapped[part + 1] + jnp.where(low_half, swapped[part], swapped[part + 2])
                )
                total = total + jnp.where(not_right, pltpu.roll(mid, LANES - 1, 1), 0.0)
                total = total + jnp.where(not_left, pltpu.roll(mid, 1, 1), 0.0)
                if link is not None:
                    at = part * held + start
                    total = total + link_sums[link, at : at + PAD]
                mass_b, damping_b, stiffness_b = diagonals[part]
                diagonal = lam_sq * mass_b + lam * damping_b + stiffness_b
                full = diagonal * mid - coupling * total
                res_packed[slot, rows, lanes] = full.astype(jnp.bfloat16)
                squares = squares + full * full
            at = slice(held + start, held + start + PAD)
            stat_out[at] += squares

    low_iota = iota((LANES, BLOCK), 0)
    row_chunk = iota((held, BLOCK), 0) & (CHUNKS - 1)

    sides = ((0, links_in, 0, 1), (1, links, 1, 0))

    def make_hot(step):
        start = pl.multiple_of(step * BLOCK, BLOCK)
        for which, lists, *ends in sides:
            for end, end_row in enumerate(ends):
                cell = lists[:, pl.ds(end_row * slots + start, BLOCK)]
                hot[2 * which + end, step] = ones_where(low_iota == (cell & (LANES - 1)))

    def link_block(step):
        start = pl.multiple_of(step * BLOCK, BLOCK)
        targets, picked, got = [], [], []
        for which, lists, source_row, target_row in sides:
            stacked = jnp.concatenate(
                [face_in[which, :, part * LANES : (part + 1) * LANES] for part in range(parts)],
                axis=0,
            )
            source = lists[:, pl.ds(source_row * slots + start, BLOCK)]
            targets.append(lists[:, pl.ds(target_row * slots + start, BLOCK)])
            rows = jnp.dot(stacked, hot[2 * which, step], preferred_element_type=jnp.float32)
            picked.append((source, rows))
        for source, rows in picked:
            high = jnp.broadcast_to(source >> 7, (held, BLOCK))
            total = jnp.zeros((held, BLOCK), jnp.float32)
            for part in range(parts):
                mine = high == row_chunk * parts + part
                total = total + jnp.where(mine, rows[part * held : (part + 1) * held], 0.0)
            got.append(
                jnp.dot(
                    chunk_ones[...], total.astype(jnp.bfloat16), preferred_element_type=jnp.float32
                )
            )
        for (which, *_), target, value in zip(sides, targets, got):
            high = jnp.broadcast_to(target >> 7, (held, BLOCK))
            placed = jnp.concatenate(
                [
                    jnp.where(high == row_chunk * parts + part, value, 0.0).astype(jnp.bfloat16)
                    for part in range(parts)
                ],
                axis=0,
            )
            link_sums[which] += lax.dot_general(
                placed,
                hot[2 * which + 1, step],
                (((1,), (1,)), ((), ())),
                preferred_element_type=jnp.float32,
            )

    rounds = meet_sem.shape[0]

    def met(round_):
        pl.semaphore_wait(meet_sem.at[round_], 2)
        if round_ + 1 < rounds:
            meet(round_ + 1)

    def plain(plane):
        stencil(plane, None)
        write_res(plane, 0)

    blocks = slots // BLOCK

    inner(0)
    send_half(2, 0)
    met(0)
    links_copy().wait_recv()
    each(0, blocks, make_hot)
    join(0)
    send_half(2, 1)
    send_tail(2)
    inner(1)
    met(1)
    close(0)
    face_copy(0).start()
    face_copy(1).start()
    send_half(3, 0)
    plain(1)
    met(2)
    face_copy(0).wait_recv()
    face_copy(1).wait_recv()
    each(0, 2, link_block)
    join(1)
    send_half(3, 1)
    send_tail(3)
    inner(2)
    each(2, 3, link_block)
    met(3)
    close(1)
    each(2, 6, plain)
    each(3, 5, link_block)
    inner(3)
    each(5, blocks, link_block)
    join(2)
    stencil(0, 0)
    write_res(0, 0)
    join(3, True)
    close(2, True)
    late = 6
    each(late, 10, lambda plane: stencil(plane, None, plane - late))
    tail = range(10, planes)
    for half in range(2):
        for side in range(2):
            close_part(3, side, half)
        for plane in tail:
            stencil(plane, 1 if plane == planes - 1 else None, plane - late, *cuts[half])

    sums = jnp.sum(stat_out[...].reshape(2 * vector_part, CHUNKS, LANES), axis=1)
    sums = jnp.sum(sums, axis=1, keepdims=True)
    spot = iota((2 * vector_part, LANES), 0) == iota((2 * vector_part, LANES), 1)
    line = jnp.sum(jnp.where(spot, sums, 0.0), axis=0, keepdims=True)
    stat_line[...] = line
    for step in sorted(range(1, count), key=distance):
        stat_copy(step).start()
    def write_late(side):
        write_eig(outer_at(2, side))
        write_eig(inner_at(3, side))
        write_eig(outer_at(3, side))

    each(0, 2, write_late)
    each(late, planes, lambda plane: write_res(plane, plane - late))

    def sent(turn):
        for side in range(2):
            for half in range(2):
                raw_copy(turn, side, half).wait_send()
            tail_copy(turn, side).wait_send()
            for half in range(2):
                mid_copy(turn, side, half).wait_send()
                last_copy(turn, side, half).wait_send()

    each(0, turns, sent)
    links_copy().wait_send()
    face_copy(0).wait_send()
    face_copy(1).wait_send()
    all_stats().wait_recv()
    for step in range(1, count):
        line = line + stat_in[step]
    norms = jnp.sqrt(line[:, vector_part : 2 * vector_part]) / jnp.sqrt(line[:, :vector_part] + 1.0)
    norm_out[...] = norms
    all_stats().wait_send()


def write_back(eig_held, res_held, norm_held, eig_out, res_out, norm_out, sem):
    copies = [
        pltpu.make_async_copy(source, target, sem.at[place])
        for place, (source, target) in enumerate(
            ((eig_held, eig_out), (res_held, res_out), (norm_held, norm_out))
        )
    ]
    for copy in copies:
        copy.start()
    for copy in copies:
        copy.wait()


def on_device(
    basis,
    coefficients,
    eigen_values,
    stiffness,
    damping,
    mass,
    link_count,
    lower_cells,
    upper_cells,
):
    count = lax.axis_size("rows")
    vector_part = eigen_values.shape[0]
    rank_part, rows_local = basis.shape
    cells = WID * WID
    planes = rows_local // cells
    slots = lower_cells.shape[1]
    held = vector_part * CHUNKS
    width = cells // CHUNKS
    rounds = (count // 2 - 1).bit_length()
    vmem = pl.BlockSpec(memory_space=pltpu.VMEM)
    anywhere = pl.BlockSpec(memory_space=pltpu.HBM)
    dma = pltpu.SemaphoreType.DMA
    pairs = planes // VECS * 2
    whole = rank_part // CHUNKS * CHUNKS

    def wire(*shape):
        return pltpu.VMEM(shape, jnp.bfloat16)

    eigvecs, residuals, norms = pl.pallas_call(
        functools.partial(kernel, count, planes, cells, vector_part, rank_part),
        out_shape=(
            pltpu.VMEM((vector_part, rows_local), jnp.bfloat16),
            pltpu.VMEM((vector_part, rows_local), jnp.bfloat16),
            pltpu.VMEM((1, vector_part), jnp.float32),
        ),
        in_specs=[anywhere] * 9,
        out_specs=(vmem, vmem, vmem),
        scratch_shapes=[
            pltpu.VMEM((planes, rank_part, cells), jnp.bfloat16),
            wire(pairs, CHUNKS, width),
            wire(pairs, whole, cells),
            wire(pairs, CHUNKS, width),
            wire(pairs, 2 * held, width),
            wire(pairs, 2 * held, width),
            pltpu.VMEM((pairs, 2 * held, width), jnp.float32),
            wire(pairs, held, width),
            wire(pairs, held, width),
            pltpu.VMEM((planes + 2, held, width), jnp.float32),
            wire(planes, held, width),
            wire(10, held, width),
            pltpu.VMEM((2, held, width), jnp.bfloat16),
            pltpu.VMEM((1, 2 * slots), jnp.int32),
            pltpu.VMEM((1, 2 * slots), jnp.int32),
            wire(4, slots // BLOCK, LANES, BLOCK),
            pltpu.VMEM((2, width // LANES * held, LANES), jnp.float32),
            pltpu.VMEM((2 * held, LANES), jnp.float32),
            pltpu.VMEM((count, 1, LANES), jnp.float32),
            pltpu.VMEM((1, LANES), jnp.float32),
            wire(2, 4 * held, CHUNKS * DEPTH),
            wire(2, 4 * held, CHUNKS * DEPTH),
            pltpu.VMEM((CHUNKS * PAD, held), jnp.bfloat16),
            pltpu.VMEM((held, held), jnp.bfloat16),
            pltpu.VMEM((3, held, LANES), jnp.float32),
            pltpu.VMEM((rows_local // LANES, LANES), jnp.float32),
            pltpu.VMEM((rows_local // LANES, LANES), jnp.float32),
            pltpu.VMEM((rows_local // LANES, LANES), jnp.float32),
            pltpu.VMEM(coefficients.shape[::-1], jnp.bfloat16),
            pltpu.VMEM((1, vector_part), jnp.float32),
            pltpu.VMEM((1, 1), jnp.int32),
            pltpu.VMEM((1, slots), jnp.int32),
            pltpu.VMEM((1, slots), jnp.int32),
            dma((8,)),
            dma((planes,)),
            dma((3, pairs)),
            dma((3, pairs)),
            dma((2, pairs)),
            dma((2, pairs)),
            dma((2, pairs)),
            dma((2, pairs)),
            dma((3,)),
            dma((3,)),
            dma((1,)),
            dma((1,)),
            pltpu.SemaphoreType.REGULAR((rounds,)),
        ],
        compiler_params=pltpu.CompilerParams(
            collective_id=0, has_side_effects=True, vmem_limit_bytes=56 * 1024 * 1024
        ),
    )(
        basis,
        coefficients.T,
        eigen_values[None, :],
        stiffness.reshape(-1, LANES),
        damping.reshape(-1, LANES),
        mass.reshape(-1, LANES),
        link_count[None, :],
        lower_cells,
        upper_cells,
    )
    eigvecs, residuals, norms = pl.pallas_call(
        write_back,
        out_shape=tuple(
            jax.ShapeDtypeStruct(held.shape, held.dtype) for held in (eigvecs, residuals, norms)
        ),
        in_specs=[vmem] * 3,
        out_specs=[pl.BlockSpec(memory_space=pl.ANY)] * 3,
        scratch_shapes=[dma((3,))],
        compiler_params=pltpu.CompilerParams(vmem_limit_bytes=1 << 20),
    )(eigvecs, residuals, norms)
    return eigvecs, residuals, norms[0]


def solution(mesh):
    placed = (
        P("vecs", "rows"),
        P(),
        P("vecs"),
        P("rows"),
        P("rows"),
        P("rows"),
        P("rows"),
        P("rows", None),
        P("rows", None),
    )
    return jax.shard_map(
        on_device,
        mesh=mesh,
        in_specs=placed,
        out_specs=(P("vecs", "rows"), P("vecs", "rows"), P("vecs")),
        check_vma=False,
    )
```
